512 devices in a mesh: ens: 16 (over x, y_hi), lat: 16 (over y_lo, z), lon: 2 (over core).
Axes of the slice: x: 4, y: 8 (y_hi: 4, y_lo: 2; y = y_hi * 2 + y_lo), z: 8, core: 2. Of those that a mesh axis runs over, the one named last changes fastest.
Arguments:
- hidden_state: bfloat16 [16, 90, 32, 720], P('ens', None, 'lat', 'lon'), may hold values from -6 to 6
- filter_coefficients: bfloat16 [9, 10, 90], replicated, may hold values from -0.21875 to 0.21875
- meridian_offset_table: int32 [3, 32], P(None, 'lat'), may hold values from 1 to 4
- function_pick_table: int32 [9, 32, 1440], P(None, 'lat', 'lon'), may hold values from 0 to 8
- observation: float32 [10, 32, 1440], P(None, 'lat', 'lon'), may hold values from -6 to 6
- latitude_cosine_factor: float32 [32], P('lat'), may hold values from 0.3 to 3
Outputs:
- latent_grad: float32 [16, 90, 32, 720], P('ens', None, 'lat', 'lon')
The draws below stay inside these ranges and needn't reach their ends.
All inputs are finite; a program needn't handle non-finite values.
Results may differ from the reference program's by a relative error of at most 0.0037.
Values may be sent and summed in bfloat16 or wider, within the bound.
A program may use at most 64 MiB of HBM per device.

```python
import math
import jax
import jax.numpy as jnp
from jax import lax

C = 90
V = 10
NLON = 1440
BASES = 9
SPAN = 4
MEMBERS = 16
NLAT = 32
LLON = 720


def set_ends(values, stream_key, least, top_value):
    longest = values.shape.index(max(values.shape))
    spots = []
    for shift in (0, 1):
        where = [jax.random.randint(jax.random.fold_in(stream_key, axis), (), 0, length) for axis, length in enumerate(values.shape)]
        where[longest] = (where[longest] + shift) % values.shape[longest]
        spots.append(tuple(where))
    return values.at[spots[0]].set(least).at[spots[1]].set(top_value)


def block_scale(own_key, shape, pieces, low, top_value):
    factor_of, own = 1.0, jax.random.fold_in(own_key, 6)
    for axis_at, blocks in pieces:
        steps = jnp.exp(jax.random.uniform(jax.random.fold_in(own, axis_at), (blocks,), jnp.float32, low / len(pieces), top_value / len(pieces)))
        factor_of = factor_of * jnp.repeat(steps, shape[axis_at] // blocks).reshape([-1 if axis == axis_at else 1 for axis in range(len(shape))])
    return factor_of


def gaussian(stream_key, dims, width, limit, split=(), held_as=jnp.bfloat16):
    drawn = width * jax.random.normal(stream_key, dims, jnp.float32)
    if split:
        drawn = drawn * block_scale(stream_key, dims, split, -0.22, 0.18)
    return jnp.clip(drawn, -limit, limit).astype(held_as)


def setup_inputs(seed: int = 0) -> dict:
    seeds = jax.random.split(jax.random.key(seed), 7)
    hidden_state = gaussian(seeds[0], (MEMBERS, C, NLAT, LLON), 1.0, 6.0, ((0, 16), (2, 16), (3, 2)))
    filter_coefficients = gaussian(seeds[1], (BASES, V, C), (BASES * C) ** -0.5, 0.21875)
    meridian_offset_table = set_ends(jax.random.randint(seeds[2], (3, NLAT), 1, SPAN + 1), jax.random.fold_in(seeds[2], 1), 1, SPAN).astype(jnp.int32)
    function_pick_table = set_ends(jax.random.randint(seeds[3], (BASES, NLAT, NLON), 0, BASES), jax.random.fold_in(seeds[3], 1), 0, BASES - 1).astype(jnp.int32)
    observation = gaussian(seeds[4], (V, NLAT, NLON), 1.0, 6.0, ((1, 16), (2, 2)), jnp.float32)
    latitude_cosine_factor = jnp.clip(jnp.exp(math.log(3.0) - 2.3025851 * jax.random.uniform(seeds[5], (NLAT,), jnp.float32) ** block_scale(seeds[5], (NLAT,), ((0, 16),), -0.2, 0.2)), 0.3, 3.0)
    return {"hidden_state": hidden_state, "filter_coefficients": filter_coefficients, "meridian_offset_table": meridian_offset_table, "function_pick_table": function_pick_table, "observation": observation, "latitude_cosine_factor": latitude_cosine_factor}


smooth_square = 0.01

def smoothed_derivative(difference):
    return difference / jnp.sqrt(difference * difference + smooth_square)

def shift_rows(values, offset):
    parallel_number = values.shape[-2]
    widths = [(0, 0)] * (values.ndim - 2)
    if offset > 0:
        padded = jnp.pad(values, widths + [(0, offset), (0, 0)])
        return padded[..., offset:offset + parallel_number, :]
    if offset < 0:
        padded = jnp.pad(values, widths + [(-offset, 0), (0, 0)])
        return padded[..., :parallel_number, :]
    return values

def predict(member_latent, filter_coefficients, meridian_offset_table, function_pick_table):
    basis_count, variables, channels = filter_coefficients.shape
    parallel_number = member_latent.shape[1]
    meridian_number = member_latent.shape[2] * 2
    latent_f32 = member_latent.astype(jnp.float32)
    halfway = 0.5 * (latent_f32 + jnp.roll(latent_f32, -1, axis=-1))
    interpolated = jnp.stack([latent_f32, halfway], axis=-1).reshape(channels, parallel_number, meridian_number).astype(jnp.bfloat16)
    product = jnp.dot(filter_coefficients.reshape(basis_count * variables, channels), interpolated.reshape(channels, -1), preferred_element_type=jnp.float32)
    product = product.reshape(basis_count, variables, parallel_number, meridian_number)
    columns = jnp.arange(meridian_number, dtype=jnp.int32)
    levels = jnp.arange(basis_count, dtype=jnp.int32)
    result = jnp.zeros((variables, parallel_number, meridian_number), jnp.float32)
    for row_step in (-1, 0, 1):
        shifted = shift_rows(product, row_step)
        for col_step in (-1, 0, 1):
            adjacent_position = 3 * (row_step + 1) + col_step + 1
            target_cols = (columns[None, :] + col_step * meridian_offset_table[row_step + 1][:, None]) % meridian_number
            picked = jnp.take_along_axis(shifted, jnp.broadcast_to(target_cols[None, None], shifted.shape), axis=3)
            picked_function = (function_pick_table[adjacent_position][None] == levels[:, None, None]).astype(jnp.float32)
            result = result + lax.optimization_barrier(jnp.sum(picked_function[:, None] * picked, axis=0))
    return result

def hidden_derivative_accum(prediction_derivative, filter_coefficients, meridian_offset_table, function_pick_table):
    basis_count, variables, channels = filter_coefficients.shape
    parallel_number = prediction_derivative.shape[1]
    meridian_number = prediction_derivative.shape[2]
    columns = jnp.arange(meridian_number, dtype=jnp.int32)
    levels = jnp.arange(basis_count, dtype=jnp.int32)
    product_grad = jnp.zeros((basis_count, variables, parallel_number, meridian_number), jnp.float32)
    for row_step in (-1, 0, 1):
        collected = jnp.zeros((basis_count, variables, parallel_number, meridian_number), jnp.float32)
        for col_step in (-1, 0, 1):
            adjacent_position = 3 * (row_step + 1) + col_step + 1
            picked_function = (function_pick_table[adjacent_position][None] == levels[:, None, None]).astype(jnp.float32)
            sample_dispersion = picked_function[:, None] * prediction_derivative[None]
            source_cols = (columns[None, :] - col_step * meridian_offset_table[row_step + 1][:, None]) % meridian_number
            collected = collected + jnp.take_along_axis(sample_dispersion, jnp.broadcast_to(source_cols[None, None], sample_dispersion.shape), axis=3)
        product_grad = product_grad + shift_rows(collected, -row_step)
    flat_weight = filter_coefficients.reshape(basis_count * variables, channels).astype(jnp.float32)
    field_grad = jnp.dot(flat_weight.T, product_grad.reshape(basis_count * variables, -1), precision=lax.Precision.HIGHEST)
    paired = field_grad.reshape(channels, parallel_number, meridian_number // 2, 2)
    even_part = paired[..., 0]
    odd_part = paired[..., 1]
    return even_part + 0.5 * odd_part + 0.5 * jnp.roll(odd_part, 1, axis=-1)

def reference(hidden_state, filter_coefficients, meridian_offset_table, function_pick_table, observation, latitude_cosine_factor):

    def decode_sample(member_latent):
        return predict(member_latent, filter_coefficients, meridian_offset_table, function_pick_table)
    prediction_fields = lax.map(decode_sample, hidden_state)
    sample_number = prediction_fields.shape[0]

    def couple_accumulated(sample_outputs):
        return lax.optimization_barrier(jnp.sum(smoothed_derivative(sample_outputs[None] - prediction_fields), axis=0))
    sample_couples = lax.map(couple_accumulated, prediction_fields)
    prediction_derivative = latitude_cosine_factor[None, None, :, None] * (smoothed_derivative(prediction_fields - observation[None]) - sample_couples / (sample_number - 1))

    def sample_reverse_sweep(member_grad):
        return hidden_derivative_accum(member_grad, filter_coefficients, meridian_offset_table, function_pick_table)
    return lax.map(sample_reverse_sweep, prediction_derivative)
```

```python
import functools

import jax
import jax.numpy as jnp
import numpy as np
from jax import lax
from jax.experimental import pallas as pl
from jax.experimental.pallas import tpu as pltpu
from jax.sharding import PartitionSpec as P

SPAN = 4
BASES = 9
LANES = 384
TILE = 128
ROWS = 24
SMOOTH = 0.01
F32 = jnp.float32
BF16 = jnp.bfloat16
MESH = pl.DeviceIdType.MESH


def expand_picks():
    rows = np.zeros((112, 32), np.float32)
    for slot in range(9):
        a = slot // 3 - 1
        for sub in range(8):
            q = (sub & 1) - a
            if 0 <= q <= 1:
                rows[8 * slot + sub, 2 * slot + q] = 1
    for i in range(3):
        rows[72 + i, 2 * i] = 1
        rows[80 + i, 2 * (6 + i) + 1] = 1
        rows[88 + 3 + i, 2 * i] = 1
        rows[96 + 3 + i, 2 * (6 + i) + 1] = 1
    return rows


def expand_weights():
    rows = np.zeros((BASES * ROWS, 96), np.float32)
    for k in range(BASES):
        for v in range(10):
            for p in range(2):
                rows[ROWS * k + 2 * v + p, 10 * k + v] = 1
    return rows


def iota(shape, dim):
    return lax.broadcasted_iota(jnp.int32, shape, dim)


def lane_roll(x, by):
    by %= x.shape[-1]
    return x if by == 0 else pltpu.roll(x, by, axis=x.ndim - 1)


def row_down(x):
    return pltpu.roll(x, 1, axis=x.ndim - 2)


def row_up(x):
    return pltpu.roll(x, x.shape[-2] - 1, axis=x.ndim - 2)


def smoothed_derivative(d):
    return d * lax.rsqrt(d * d + SMOOTH)


def shifted(pair, sign, steps):
    rolled = {}

    def at(parity, by):
        if (parity, by) not in rolled:
            rolled[parity, by] = lane_roll(pair[parity], -by)
        return rolled[parity, by]

    steps = jnp.broadcast_to(steps, pair[0].shape)
    out = []
    for parity in (0, 1):
        result = None
        for n in range(1, SPAN + 1):
            column = parity + sign * n
            value = at(column % 2, column // 2)
            result = value if result is None else jnp.where(steps == float(n), value, result)
        out.append(result)
    return out


def edge_of(x):
    lane = iota((*x.shape[:-1], TILE), x.ndim - 1)
    return jnp.where(lane < 64, x[..., :TILE], x[..., 2 * TILE :])


def extended(x, edge):
    lane = iota(edge.shape, edge.ndim - 1)
    last = jnp.where(
        lane < 104, x[..., 2 * TILE :], jnp.where(lane < 112, lane_roll(edge, 104), lane_roll(edge, 24))
    )
    return jnp.concatenate([x[..., : 2 * TILE], last], axis=-1)


def kernel(
    nx, ny, nlat, off_ref, cos_ref, x_ref, w_ref, pk_ref, obs_ref, s1_ref, ex_ref, out_ref,
    xpar, prod, qp, mask, csum, fsel, pgrad, su, sd, ru, rd, zu, zd, rzu, rzd,
    qpe, rqpe, own, yblk, xblk, fe, rfe, f0, f1, r0, r1, f0e, f1e, r0e, r1e, send_sem, recv_sem,
):
    ens = lax.axis_index("ens")
    lat = lax.axis_index("lat")
    lon = lax.axis_index("lon")
    ex, ey = ens // ny, ens % ny
    up = (lat + nlat - 1) % nlat
    down = (lat + 1) % nlat
    partner = 1 - lon
    have_up = jnp.where(lat > 0, 1.0, 0.0).astype(F32)
    have_down = jnp.where(lat < nlat - 1, 1.0, 0.0).astype(F32)

    def x_peer(d):
        return ((ex + d) % nx) * ny + ey

    def y_peer(d):
        return ex * ny + (ey + d) % ny

    def target(e=None, t=None, n=None):
        return (ens if e is None else e, lat if t is None else t, lon if n is None else n)

    sems = [0]

    def remote(src, dst, device):
        i = sems[0]
        sems[0] += 1
        return pltpu.make_async_remote_copy(
            src_ref=src, dst_ref=dst, send_sem=send_sem.at[i], recv_sem=recv_sem.at[i],
            device_id=device, device_id_type=MESH,
        )

    barrier = pltpu.get_barrier_semaphore()
    peers = [target(n=partner)]
    peers += [target(t=t, n=n) for t in (up, down) for n in (lon, partner)]
    peers += [target(e=x_peer(d)) for d in range(1, nx)] + [target(e=y_peer(d)) for d in range(1, ny)]
    for device in peers:
        pl.semaphore_signal(barrier, inc=1, device_id=device, device_id_type=MESH)

    pick = iota((256, 256), 0) - 2 * iota((256, 256), 1)
    half = iota((256, 256), 1)
    select = jnp.where((pick == jnp.where(half < TILE, 0, -255)), 1.0, 0.0).astype(BF16)
    rows = jnp.dot(ex_ref[...], pk_ref[...], preferred_element_type=F32).astype(BF16)
    obs = obs_ref[...]
    obs_hi = obs.astype(BF16)
    obs_lo = (obs - obs_hi.astype(F32)).astype(BF16)
    obs_e, obs_o = [], []
    row8 = iota((8, TILE), 0)
    for block in range(3):
        wide = slice(256 * block, 256 * block + 256)
        tile = slice(TILE * block, TILE * block + TILE)
        got = jnp.dot(rows[:, wide], select, preferred_element_type=F32)
        for slot in range(9):
            qp[0, slot, :, tile] = got[8 * slot : 8 * slot + 8, :TILE]
            qp[1, slot, :, tile] = got[8 * slot : 8 * slot + 8, TILE:]
        su[:, tile] = jnp.where(row8 == 6, off_ref[0, 0], got[72:80, :TILE] + got[88:96, TILE:])
        sd[:, tile] = jnp.where(row8 == 6, off_ref[2, 1], got[80:88, :TILE] + got[96:104, TILE:])
        both = jnp.dot(obs_hi[:, wide], select, preferred_element_type=F32) + jnp.dot(
            obs_lo[:, wide], select, preferred_element_type=F32
        )
        obs_e.append(both[:, :TILE])
        obs_o.append(both[:, TILE:])
    obs = jnp.concatenate([jnp.concatenate(obs_e, axis=1), jnp.concatenate(obs_o, axis=1)], axis=0)

    pl.semaphore_wait(barrier, len(peers))
    started = []

    def go(src, dst, device):
        copy = remote(src, dst, device)
        copy.start()
        started.append(copy)
        return copy

    c_x = go(x_ref, xpar, target(n=partner))
    c_up = go(su, rd, target(t=up))
    c_down = go(sd, ru, target(t=down))

    spread = jnp.dot(s1_ref[...], w_ref[...], preferred_element_type=F32).astype(BF16)
    s2 = jnp.where(iota((TILE, 192), 1) // 2 == iota((TILE, 192), 0), 1.0, 0.0).astype(BF16)
    wf = jnp.dot(spread, s2, preferred_element_type=F32)
    wf = jnp.where(iota(wf.shape, 0) % 2 == iota(wf.shape, 1) % 2, wf, 0.0).astype(BF16)
    s2t = jnp.where(iota((192, TILE), 0) // 2 == iota((192, TILE), 1), 1.0, 0.0).astype(BF16)
    wb = lax.dot_general(s2t, spread, (((1,), (1,)), ((), ())), preferred_element_type=F32)
    wb = jnp.where(iota(wb.shape, 0) % 2 == iota(wb.shape, 1) % 2, wb, 0.0).astype(BF16)

    c_x.wait_recv()
    latent = extended(x_ref[...].astype(F32), edge_of(xpar[...].astype(F32)))
    halfway = 0.5 * (latent + lane_roll(latent, -1))
    for parity, x in enumerate((latent, halfway)):
        got = jnp.dot(wf, x.astype(BF16), preferred_element_type=F32)
        prod[parity] = got.reshape(BASES, 3, 8, LANES)

    c_up.wait_recv()
    c_down.wait_recv()
    even = iota((8, LANES), 0) % 2 == 0

    def spread_row(ref, i):
        return jnp.broadcast_to(ref[i : i + 1, :], (8, LANES))

    steps = {
        -1: jnp.where(even, off_ref[0, 1], spread_row(rd, 6)),
        0: None,
        1: jnp.where(even, spread_row(ru, 6), off_ref[2, 0]),
    }
    own0 = jnp.where(even, off_ref[1, 0], off_ref[1, 1])
    steps[0] = own0
    for parity in (0, 1):
        for i in range(3):
            qp[parity, 6 + i] = jnp.where(even, spread_row(ru, 3 * parity + i), qp[parity, 6 + i])
            qp[parity, i] = jnp.where(even, qp[parity, i], spread_row(rd, 3 * parity + i))
    for parity in (0, 1):
        qpe[parity] = edge_of(qp[parity])
    c_q = go(qpe, rqpe, target(n=partner))

    def build_masks(source):
        for a in (-1, 0, 1):
            for b in (-1, 0, 1):
                slot = 3 * (a + 1) + b + 1
                pair = source(slot)
                if b:
                    pair = shifted(pair, -b, steps[a])
                for parity in (0, 1):
                    mask[parity, slot] = pair[parity]

    build_masks(lambda slot: [qp[0, slot], qp[1, slot]])

    for parity in (0, 1):
        for t in range(3):
            tile = slice(TILE * t, TILE * t + TILE)
            values = [prod[parity, k, :, :, tile] for k in range(BASES)]
            for slot in range(9):
                want = jnp.broadcast_to(mask[parity, slot, :, tile][None], (3, 8, TILE))
                total = jnp.where(want == 0.0, values[0], 0.0)
                for k in range(1, BASES):
                    total = jnp.where(want == float(k), values[k], total)
                csum[parity, slot, :, :, tile] = total

    def target_sum(a):
        total = [csum[0, 3 * (a + 1) + 1], csum[1, 3 * (a + 1) + 1]]
        for b in (-1, 1):
            slot = 3 * (a + 1) + b + 1
            moved = shifted([csum[0, slot], csum[1, slot]], b, steps[a])
            total = [x + y for x, y in zip(total, moved)]
        return total

    even3 = iota((3, 8, LANES), 1) % 2 == 0
    to_up = target_sum(1)
    to_down = target_sum(-1)
    zu[...] = jnp.where(even3, to_up[0], row_down(to_up[1]))
    zd[...] = jnp.where(even3, row_up(to_down[0]), to_down[1])
    c_zu = go(zu, rzu, target(t=up))
    c_zd = go(zd, rzd, target(t=down))
    middle = target_sum(0)
    local = [
        middle[parity] + jnp.where(even3, row_up(to_up[parity]), row_down(to_down[parity])) for parity in (0, 1)
    ]
    c_zu.wait_recv()
    c_zd.wait_recv()
    from_down = rzu[...] * have_down
    from_up = rzd[...] * have_up
    pred = [
        local[0] + jnp.where(even3, from_up, row_down(from_down)),
        local[1] + jnp.where(even3, row_up(from_up), from_down),
    ]
    pred = jnp.concatenate([x.reshape(ROWS, LANES) for x in pred], axis=0)
    own[...] = pred.astype(BF16)

    c_y = [go(own, yblk.at[d - 1], target(e=y_peer(d))) for d in range(1, ny)]
    c_xs = [go(own, xblk.at[0, d - 1], target(e=x_peer(d))) for d in range(1, nx)]
    pair_total = jnp.zeros_like(pred)
    relayed = [c_xs]
    for d in range(1, ny):
        c_y[d - 1].wait_recv()
        relayed.append([go(yblk.at[d - 1], xblk.at[d, e - 1], target(e=x_peer(e))) for e in range(1, nx)])

    c_q.wait_recv()
    build_masks(lambda slot: [extended(qp[parity, slot], rqpe[parity, slot]) for parity in (0, 1)])

    for d in range(1, ny):
        pair_total += smoothed_derivative(pred - yblk[d - 1].astype(F32))
    for d in range(ny):
        for e in range(1, nx):
            relayed[d][e - 1].wait_recv()
            pair_total += smoothed_derivative(pred - xblk[d, e - 1].astype(F32))

    factor = jnp.where(iota(pred.shape, 0) % 2 == 0, cos_ref[0], cos_ref[1])
    grad = factor * (smoothed_derivative(pred - obs) - pair_total * (1.0 / (nx * ny - 1)))
    grad = [grad[:ROWS].reshape(3, 8, LANES), grad[ROWS:].reshape(3, 8, LANES)]
    f0[...] = jnp.where(even3, grad[0], row_down(grad[1]))
    f1[...] = jnp.where(even3, row_up(grad[0]), grad[1])
    f0e[...] = edge_of(f0[...])
    f1e[...] = edge_of(f1[...])
    for parity in (0, 1):
        fe[parity] = edge_of(grad[parity])
    c_f = [
        go(f0, r0, target(t=up)),
        go(f1, r1, target(t=down)),
        go(f0e, r0e, target(t=up, n=partner)),
        go(f1e, r1e, target(t=down, n=partner)),
        go(fe, rfe, target(n=partner)),
    ]

    def around(own_pair, below, above):
        is_even = iota(below.shape, 1) % 2 == 0
        return {
            1: [
                jnp.where(is_even, above, row_down(own_pair[0])),
                jnp.where(is_even, row_up(above), row_down(own_pair[1])),
            ],
            0: own_pair,
            -1: [
                jnp.where(is_even, row_up(own_pair[0]), row_down(below)),
                jnp.where(is_even, row_up(own_pair[1]), below),
            ],
        }

    for copy in c_f:
        copy.wait_recv()
    seen = around(grad, r0[...] * have_down, r1[...] * have_up)
    edges = around([rfe[0], rfe[1]], r0e[...] * have_down, r1e[...] * have_up)
    for a in (-1, 0, 1):
        wide = [extended(x, edge) for x, edge in zip(seen[a], edges[a])]
        for b in (-1, 0, 1):
            slot = 3 * (a + 1) + b + 1
            pair = shifted(wide, -b, steps[a]) if b else wide
            for parity in (0, 1):
                fsel[parity, slot] = pair[parity]

    for parity in (0, 1):
        for t in range(3):
            tile = slice(TILE * t, TILE * t + TILE)
            values = [fsel[parity, slot, :, :, tile] for slot in range(9)]
            wants = [jnp.broadcast_to(mask[parity, slot, :, tile][None], (3, 8, TILE)) for slot in range(9)]
            for k in range(BASES):
                total = jnp.where(wants[0] == float(k), values[0], 0.0)
                for slot in range(1, 9):
                    total = total + jnp.where(wants[slot] == float(k), values[slot], 0.0)
                pgrad[parity, k, :, :, tile] = total

    odd = pgrad[1].reshape(BASES * ROWS, LANES)
    folded = pgrad[0].reshape(BASES * ROWS, LANES) + 0.5 * (odd + lane_roll(odd, 1))
    out_ref[...] = jnp.dot(wb, folded.astype(BF16), preferred_element_type=F32)

    for copy in started:
        copy.wait_send()


def on_device(sizes, hidden_state, filter_coefficients, meridian_offset_table, function_pick_table, observation, latitude_cosine_factor):
    nx, ny, nlat = sizes
    channels = hidden_state.shape[1]
    columns = hidden_state.shape[3]
    x = jnp.pad(hidden_state.reshape(2 * channels, columns), ((0, 192 - 2 * channels), (0, LANES - columns)))
    weights = jnp.pad(filter_coefficients.reshape(90, 90), ((0, 6), (0, 38)))
    picks = jnp.pad(function_pick_table.reshape(18, 2 * columns).astype(BF16), ((0, 14), (0, 768 - 2 * columns)))
    obs = jnp.pad(observation.reshape(20, 2 * columns), ((0, 4), (0, 768 - 2 * columns)))
    smem = pl.BlockSpec(memory_space=pltpu.SMEM)
    vmem = pl.BlockSpec(memory_space=pltpu.VMEM)
    row = pltpu.VMEM((8, LANES), F32)
    field = pltpu.VMEM((3, 8, LANES), F32)
    edge = pltpu.VMEM((3, 8, TILE), F32)
    copies = 11 + (ny - 1) + ny * (nx - 1)
    out = pl.pallas_call(
        functools.partial(kernel, nx, ny, nlat),
        out_shape=jax.ShapeDtypeStruct((192, LANES), F32),
        in_specs=[smem, smem] + [vmem] * 6,
        out_specs=vmem,
        scratch_shapes=[
            pltpu.VMEM((192, LANES), BF16),
            pltpu.VMEM((2, 9, 3, 8, LANES), F32),
            pltpu.VMEM((2, 9, 8, LANES), F32),
            pltpu.VMEM((2, 9, 8, LANES), F32),
            pltpu.VMEM((2, 9, 3, 8, LANES), F32),
            pltpu.VMEM((2, 9, 3, 8, LANES), F32),
            pltpu.VMEM((2, 9, 3, 8, LANES), F32),
            row, row, row, row,
            field, field, field, field,
            pltpu.VMEM((2, 9, 8, TILE), F32),
            pltpu.VMEM((2, 9, 8, TILE), F32),
            pltpu.VMEM((2 * ROWS, LANES), BF16),
            pltpu.VMEM((ny - 1, 2 * ROWS, LANES), BF16),
            pltpu.VMEM((ny, nx - 1, 2 * ROWS, LANES), BF16),
            pltpu.VMEM((2, 3, 8, TILE), F32),
            pltpu.VMEM((2, 3, 8, TILE), F32),
            field, field, field, field,
            edge, edge, edge, edge,
            pltpu.SemaphoreType.DMA((copies,)),
            pltpu.SemaphoreType.DMA((copies,)),
        ],
        compiler_params=pltpu.CompilerParams(collective_id=0, has_side_effects=True),
    )(
        meridian_offset_table.astype(F32),
        latitude_cosine_factor,
        x,
        weights,
        picks,
        obs,
        jnp.asarray(expand_weights(), BF16),
        jnp.asarray(expand_picks(), BF16),
    )
    return out[: 2 * channels, :columns].reshape(1, channels, 2, columns)


def solution(mesh):
    members = mesh.shape["ens"]
    nx = 4 if members % 4 == 0 and members > 4 else 2
    return jax.shard_map(
        functools.partial(on_device, (nx, members // nx, mesh.shape["lat"])),
        mesh=mesh,
        in_specs=(
            P("ens", None, "lat", "lon"),
            P(),
            P(None, "lat"),
            P(None, "lat", "lon"),
            P(None, "lat", "lon"),
            P("lat"),
        ),
        out_specs=P("ens", None, "lat", "lon"),
        check_vma=False,
    )
```

```python
import functools

import jax
import jax.numpy as jnp
import numpy as np
from jax import lax
from jax.experimental import pallas as pl
from jax.experimental.pallas import tpu as pltpu
from jax.sharding import PartitionSpec as P

SPAN = 4
BASES = 9
LANES = 384
TILE = 128
ROWS = 24
SMOOTH = 0.01
F32 = jnp.float32
BF16 = jnp.bfloat16
MESH = pl.DeviceIdType.MESH
HALO = BF16
SUMS = F32
Y_RELAY = False
X_RELAY = ()


def expand_picks():
    rows = np.zeros((80, 18), np.float32)
    for i in range(3):
        for sub in range(8):
            rows[8 * i + sub, 2 * (3 + i) + (sub & 1)] = 1
            rows[24 + 8 * i + sub, 2 * (6 + i) if sub & 1 else 2 * i + 1] = 1
        rows[48 + i, 2 * i] = 1
        rows[56 + i, 2 * (6 + i) + 1] = 1
        rows[64 + 3 + i, 2 * i] = 1
        rows[72 + 3 + i, 2 * (6 + i) + 1] = 1
    return rows


def iota(shape, dim):
    return lax.broadcasted_iota(jnp.int32, shape, dim)


def swapped(x):
    return jnp.where(iota(x.shape, x.ndim - 2) % 2 == 0, row_up(x), row_down(x))


def packed(pair):
    middle = jnp.where(iota((8, LANES), 0) < 4, pair[0][2], pltpu.roll(pair[1][2], 4, axis=0))
    return jnp.concatenate([pair[0][:2], middle[None], pair[1][:2]], axis=0)


def unpacked(x):
    return [x[:3], jnp.concatenate([x[3:], pltpu.roll(x[2], 4, axis=0)[None]], axis=0)]


def lane_roll(x, by):
    by %= x.shape[-1]
    return x if by == 0 else pltpu.roll(x, by, axis=x.ndim - 1)


def row_down(x):
    return pltpu.roll(x, 1, axis=x.ndim - 2)


def row_up(x):
    return pltpu.roll(x, x.shape[-2] - 1, axis=x.ndim - 2)


def smoothed_derivative(d):
    return d * lax.rsqrt(d * d + SMOOTH)


def shifted(pair, sign, steps):
    rolled = {}

    def at(parity, by):
        if (parity, by) not in rolled:
            rolled[parity, by] = lane_roll(pair[parity], -by)
        return rolled[parity, by]

    steps = jnp.broadcast_to(steps, pair[0].shape)
    out = []
    for parity in (0, 1):
        result = None
        for n in range(1, SPAN + 1):
            column = parity + sign * n
            value = at(column % 2, column // 2)
            result = value if result is None else jnp.where(steps == float(n), value, result)
        out.append(result)
    return out


def edge_of(x):
    lane = iota((*x.shape[:-1], TILE), x.ndim - 1)
    return jnp.where(lane < 64, x[..., :TILE], x[..., 2 * TILE :])


def extended(x, edge):
    lane = iota(edge.shape, edge.ndim - 1)
    last = jnp.where(
        lane < 104, x[..., 2 * TILE :], jnp.where(lane < 112, lane_roll(edge, 104), lane_roll(edge, 24))
    )
    return jnp.concatenate([x[..., : 2 * TILE], last], axis=-1)


def kernel(
    nx, ny, nlat, off_hbm, cos_hbm, x_hbm, w_hbm, pk_hbm, obs_hbm, ex_hbm, pg_ref, wb_ref,
    off_ref, cos_ref, x_raw, w_ref, pk_ref, obs_ref, ex_ref, in_sem, x_par, x_pad, obs_tmp, prod, qp, mask, csum, fsel, pgrad, su, sd, r_picks, zu, zd, r_sums,
    qpe, rqpe, own, yblk, xblk, fe, rfe, f0, f1, r_grad, f0e, f1e, r_rim, send_sem, recv_sem,
):
    ens = lax.axis_index("ens")
    lat = lax.axis_index("lat")
    lon = lax.axis_index("lon")
    ex, ey = ens // ny, ens % ny
    has_up = (lat + nlat - 1) // nlat
    has_down = (2 * nlat - 2 - lat) // nlat
    partner = 1 - lon
    have_up = has_up.astype(F32)
    have_down = has_down.astype(F32)
    up = {"t": lat - has_up, "n": has_up * lon + (1 - has_up) * partner}
    down = {"t": lat + has_down, "n": has_down * lon + (1 - has_down) * partner}
    up_partner = {"t": lat - has_up, "n": partner}
    down_partner = {"t": lat + has_down, "n": partner}

    def x_peer(d):
        return ((ex + d) % nx) * ny + ey

    def y_peer(d):
        return ex * ny + (ey + d) % ny

    def target(e=None, t=None, n=None):
        return (ens if e is None else e, lat if t is None else t, lon if n is None else n)

    def step_of(a, q):
        return off_ref[q, a].astype(F32)

    sems = [0]

    def remote(src, dst, device):
        i = sems[0]
        sems[0] += 1
        return pltpu.make_async_remote_copy(
            src_ref=src, dst_ref=dst, send_sem=send_sem.at[i], recv_sem=recv_sem.at[i],
            device_id=device, device_id_type=MESH,
        )

    barrier = pltpu.get_barrier_semaphore()
    peers = [target(n=partner)]
    peers += [target(**where) for where in (up, down, up_partner, down_partner)]
    peers += [target(e=x_peer(d)) for d in range(1, nx)] + [target(e=y_peer(d)) for d in range(1, ny)]
    for device in peers:
        pl.semaphore_signal(barrier, inc=1, device_id=device, device_id_type=MESH)

    inputs = {}
    pairs = [
        ("ex", ex_hbm, ex_ref), ("pk", pk_hbm, pk_ref), ("off", off_hbm, off_ref), ("x", x_hbm, x_raw),
        ("w", w_hbm, w_ref), ("obs", obs_hbm, obs_ref), ("cos", cos_hbm, cos_ref),
    ]
    for i, (name, src, dst) in enumerate(pairs):
        inputs[name] = pltpu.make_async_copy(src, dst, in_sem.at[i])
        inputs[name].start()

    pick = iota((256, 256), 0) - 2 * iota((256, 256), 1)
    half = iota((256, 256), 1)
    select = jnp.where((pick == jnp.where(half < TILE, 0, -255)), 1.0, 0.0).astype(BF16)
    columns = pk_ref.shape[2]
    widths = [slice(256 * block, min(256 * block + 256, columns)) for block in range(3)]
    inputs["ex"].wait()
    inputs["pk"].wait()
    picks = pk_ref[...].astype(F32).reshape(18, columns).astype(BF16)
    rows = jnp.dot(ex_ref[...], picks, preferred_element_type=F32).astype(BF16)
    inputs["off"].wait()
    row8 = iota((8, TILE), 0)
    for block in range(3):
        wide = widths[block]
        part = select[: wide.stop - wide.start]
        tile = slice(TILE * block, TILE * block + TILE)
        got = jnp.dot(rows[:, wide], part, preferred_element_type=F32)
        for slot in range(6):
            qp[0, slot, :, tile] = got[8 * slot : 8 * slot + 8, :TILE]
            qp[1, slot, :, tile] = got[8 * slot : 8 * slot + 8, TILE:]
        su[:, tile] = jnp.where(row8 == 6, step_of(0, 0), got[48:56, :TILE] + got[64:72, TILE:])
        sd[:, tile] = jnp.where(row8 == 6, step_of(2, 1), got[56:64, :TILE] + got[72:80, TILE:])
    pl.semaphore_wait(barrier, len(peers))
    started = []

    def go(src, dst, device):
        copy = remote(src, dst, device)
        copy.start()
        started.append(copy)
        return copy

    def halo(to_up, to_down, into, where_up, where_down):
        base = sems[0]
        sems[0] += 2
        slots = [(to_up, where_up, has_up), (to_down, where_down, 1 - has_down)]
        arrivals = []
        for i, (src, where, slot) in enumerate(slots):
            def copy(index, src=src, where=where, i=i):
                return pltpu.make_async_remote_copy(
                    src_ref=src, dst_ref=into.at[index], send_sem=send_sem.at[base + i],
                    recv_sem=recv_sem.at[base + index], device_id=target(**where), device_id_type=MESH,
                )

            out = copy(slot)
            out.start()
            started.append(out)
            arrivals.append(copy(i))
        return arrivals

    c_picks = halo(su, sd, r_picks, up, down)
    inputs["x"].wait()
    c_x = go(x_raw, x_par, target(n=partner))

    inputs["w"].wait()
    latents = 2 * x_raw.shape[0]
    one = jnp.where(iota((ROWS, 10), 0) // 2 == iota((ROWS, 10), 1), 1.0, 0.0).astype(BF16)
    spread = [jnp.dot(one, w_ref[k], preferred_element_type=F32) for k in range(BASES)]
    spread = jnp.concatenate(spread, axis=0).astype(BF16)
    shape = (w_ref.shape[2], latents)
    s2 = jnp.where(iota(shape, 1) // 2 == iota(shape, 0), 1.0, 0.0).astype(BF16)
    wf = jnp.dot(spread, s2, preferred_element_type=F32)
    wf = jnp.where(iota(wf.shape, 0) % 2 == iota(wf.shape, 1) % 2, wf, 0.0).astype(BF16)
    s2t = jnp.where(iota(shape[::-1], 0) // 2 == iota(shape[::-1], 1), 1.0, 0.0).astype(BF16)
    wb = lax.dot_general(s2t, spread, (((1,), (1,)), ((), ())), preferred_element_type=F32)
    wb_ref[...] = jnp.where(iota(wb.shape, 0) % 2 == iota(wb.shape, 1) % 2, wb, 0.0).astype(BF16)

    inputs["obs"].wait()
    obs = obs_ref[...].reshape(20, columns)
    obs_hi = obs.astype(BF16)
    obs_lo = (obs - obs_hi.astype(F32)).astype(BF16)
    obs_tmp[...] = jnp.zeros_like(obs_tmp)
    for block in range(3):
        wide = widths[block]
        part = select[: wide.stop - wide.start]
        tile = slice(TILE * block, TILE * block + TILE)
        both = jnp.dot(obs_hi[:, wide], part, preferred_element_type=F32) + jnp.dot(
            obs_lo[:, wide], part, preferred_element_type=F32
        )
        obs_tmp[: obs.shape[0], tile] = both[:, :TILE]
        obs_tmp[ROWS : ROWS + obs.shape[0], tile] = both[:, TILE:]
    inputs["cos"].wait()

    c_x.wait_recv()
    sector = []
    for i, raw in enumerate((x_raw, x_par)):
        x_pad[i, :, 2 * TILE :] = jnp.zeros((latents, TILE), BF16)
        x_pad[i, :, : columns // 2] = raw[...].reshape(latents, columns // 2)
        sector.append(x_pad[i].astype(F32))
    latent = extended(sector[0], edge_of(sector[1]))
    halfway = 0.5 * (latent + lane_roll(latent, -1))
    for parity, x in enumerate((latent, halfway)):
        got = jnp.dot(wf, x.astype(BF16), preferred_element_type=F32)
        prod[parity] = got.reshape(BASES, 3, 8, LANES)

    even = iota((8, LANES), 0) % 2 == 0
    even3 = iota((3, 8, LANES), 1) % 2 == 0
    steps = [
        jnp.where(even, step_of(1, 0), step_of(1, 1)),
        jnp.where(even, step_of(0, 1), step_of(2, 0)),
        None,
    ]

    def build_masks(kind, source):
        for b in (-1, 0, 1):
            slot = 3 * kind + b + 1
            pair = source(slot)
            if b:
                pair = shifted(pair, -b, steps[kind])
            for parity in (0, 1):
                mask[parity, slot] = pair[parity]

    def own_columns(slot):
        return [qp[0, slot], qp[1, slot]]

    def all_columns(slot):
        return [extended(qp[parity, slot], rqpe[parity, slot]) for parity in (0, 1)]

    def pick_products(slots):
        for parity in (0, 1):
            for t in range(3):
                tile = slice(TILE * t, TILE * t + TILE)
                values = [prod[parity, k, :, :, tile] for k in range(BASES)]
                for slot in slots:
                    want = jnp.broadcast_to(mask[parity, slot, :, tile][None], (3, 8, TILE))
                    total = jnp.where(want == 0.0, values[0], 0.0)
                    for k in range(1, BASES):
                        total = jnp.where(want == float(k), values[k], total)
                    csum[parity, slot, :, :, tile] = total

    def target_sum(kind):
        total = [csum[0, 3 * kind + 1], csum[1, 3 * kind + 1]]
        for b in (-1, 1):
            slot = 3 * kind + b + 1
            moved = shifted([csum[0, slot], csum[1, slot]], b, steps[kind])
            total = [x + y for x, y in zip(total, moved)]
        return total

    for kind in (0, 1):
        build_masks(kind, own_columns)
    pick_products(range(6))
    local = [x + swapped(y) for x, y in zip(target_sum(0), target_sum(1))]

    for copy in c_picks:
        copy.wait_recv()

    def spread_row(i):
        return jnp.where(
            even,
            jnp.broadcast_to(r_picks[0, i : i + 1, :], (8, LANES)),
            jnp.broadcast_to(r_picks[1, i : i + 1, :], (8, LANES)),
        )

    steps[2] = spread_row(6)
    for parity in (0, 1):
        for i in range(3):
            qp[parity, 6 + i] = spread_row(3 * parity + i)
    build_masks(2, own_columns)
    pick_products(range(6, 9))
    away = target_sum(2)
    zu[...] = jnp.where(even3, away[0], row_down(away[1])).reshape(ROWS, LANES).astype(zu.dtype)
    zd[...] = jnp.where(even3, row_up(away[0]), away[1]).reshape(ROWS, LANES).astype(zd.dtype)
    c_sums = halo(zu, zd, r_sums, up, down)
    for parity in (0, 1):
        qpe[parity] = edge_of(qp[parity])
    c_q = go(qpe, rqpe, target(n=partner))
    for copy in c_sums:
        copy.wait_recv()
    from_up = r_sums[0].astype(F32).reshape(3, 8, LANES) * have_up
    from_down = r_sums[1].astype(F32).reshape(3, 8, LANES) * have_down
    pred = [
        local[0] + jnp.where(even3, from_up, row_down(from_down)),
        local[1] + jnp.where(even3, row_up(from_up), from_down),
    ]
    mine = packed(pred)
    own[...] = mine.reshape(40, LANES).astype(BF16)

    def terms(ref):
        return smoothed_derivative(mine - ref[...].astype(F32).reshape(5, 8, LANES))

    def spread_along(block, slots, peer, relay):
        copies = [go(block, slots[0], peer(1)), go(block, slots[1], peer(-1))]
        if not relay and len(slots) > 2:
            copies.append(go(block, slots[2], peer(2)))
        return copies

    def pass_on(slots, peer, relay, copies):
        for i in (0, 1):
            copies[i].wait_recv()
            if relay:
                half = pl.ds(0, 24) if i == 0 else pl.ds(24, 16)
                copies.append(go(slots[i].at[half], slots[2].at[half], peer(1 if i == 0 else -1)))

    if nx == 4:
        def x_to(d):
            return target(e=x_peer(d % nx))

        def y_to(d):
            return target(e=y_peer(d % ny))

        y_slots = [yblk.at[i] for i in range(3)]
        x_slots = [[xblk.at[j, i] for i in range(3)] for j in range(4)]
        c_y = spread_along(own, y_slots, y_to, Y_RELAY)
        c_xs = [spread_along(own, x_slots[0], x_to, 0 in X_RELAY)]
        c_q.wait_recv()
        for kind in range(3):
            build_masks(kind, all_columns)
        pass_on(x_slots[0], x_to, 0 in X_RELAY, c_xs[0])
        pass_on(y_slots, y_to, Y_RELAY, c_y)
        for j in (1, 2):
            c_xs.append(spread_along(y_slots[j - 1], x_slots[j], x_to, j in X_RELAY))
        for copy in c_y[2:]:
            copy.wait_recv()
        c_xs.append(spread_along(y_slots[2], x_slots[3], x_to, 3 in X_RELAY))
        pair_total = terms(x_slots[0][0]) + terms(x_slots[0][1])
        for j in (1, 2, 3):
            pass_on(x_slots[j], x_to, j in X_RELAY, c_xs[j])
            pair_total += terms(y_slots[j - 1]) + terms(x_slots[j][0]) + terms(x_slots[j][1])
        for j in range(4):
            for copy in c_xs[j][2:]:
                copy.wait_recv()
            pair_total += terms(x_slots[j][2])
    else:
        c_y = [go(own, yblk.at[d - 1], target(e=y_peer(d))) for d in range(1, ny)]
        relayed = [[go(own, xblk.at[0, d - 1], target(e=x_peer(d))) for d in range(1, nx)]]
        pair_total = jnp.zeros_like(mine)
        for d in range(1, ny):
            c_y[d - 1].wait_recv()
            relayed.append([go(yblk.at[d - 1], xblk.at[d, e - 1], target(e=x_peer(e))) for e in range(1, nx)])
            pair_total += terms(yblk.at[d - 1])
        c_q.wait_recv()
        for kind in range(3):
            build_masks(kind, all_columns)
        for d in range(ny):
            for e in range(1, nx):
                relayed[d][e - 1].wait_recv()
                pair_total += terms(xblk.at[d, e - 1])
    pair_total = unpacked(pair_total)

    factor = jnp.where(even3, cos_ref[0], cos_ref[1])
    grad = []
    for parity in (0, 1):
        miss = pred[parity] - obs_tmp[ROWS * parity : ROWS * (parity + 1)].reshape(3, 8, LANES)
        grad.append(factor * (smoothed_derivative(miss) - pair_total[parity] * (1.0 / (nx * ny - 1))))
        fe[parity] = edge_of(grad[parity])
    lower = jnp.where(even3, grad[0], row_down(grad[1]))
    upper = jnp.where(even3, row_up(grad[0]), grad[1])
    f0[...] = lower.reshape(ROWS, LANES).astype(f0.dtype)
    f1[...] = upper.reshape(ROWS, LANES).astype(f1.dtype)
    f0e[...] = edge_of(lower).reshape(ROWS, TILE).astype(f0e.dtype)
    f1e[...] = edge_of(upper).reshape(ROWS, TILE).astype(f1e.dtype)
    c_fe = go(fe, rfe, target(n=partner))
    c_f = halo(f0, f1, r_grad, up, down) + halo(f0e, f1e, r_rim, up_partner, down_partner)

    def spread_gradient(kind, wide):
        for b in (-1, 0, 1):
            pair = shifted(wide, -b, steps[kind]) if b else wide
            for parity in (0, 1):
                fsel[parity, 3 * kind + b + 1] = pair[parity]

    def add_gradient(slots, first):
        for parity in (0, 1):
            for t in range(3):
                tile = slice(TILE * t, TILE * t + TILE)
                values = [fsel[parity, slot, :, :, tile] for slot in slots]
                wants = [jnp.broadcast_to(mask[parity, slot, :, tile][None], (3, 8, TILE)) for slot in slots]
                for k in range(BASES):
                    chosen = [jnp.where(want == float(k), value, 0.0) for want, value in zip(wants, values)]
                    if not first:
                        chosen.append(pgrad[parity, k, :, :, tile])
                    while len(chosen) > 1:
                        chosen = [x + y for x, y in zip(chosen[::2], chosen[1::2])] + chosen[len(chosen) & ~1 :]
                    pgrad[parity, k, :, :, tile] = chosen[0]

    c_fe.wait_recv()
    wide = [extended(grad[parity], rfe[parity]) for parity in (0, 1)]
    spread_gradient(0, wide)
    spread_gradient(1, [swapped(x) for x in wide])
    add_gradient(range(6), True)

    def neighbours(below, above):
        below = below.astype(F32).reshape(3, 8, -1) * have_down
        above = above.astype(F32).reshape(3, 8, -1) * have_up
        is_even = iota(below.shape, 1) % 2 == 0
        return [jnp.where(is_even, above, row_down(below)), jnp.where(is_even, row_up(above), below)]

    for copy in c_f:
        copy.wait_recv()
    inner, rim = neighbours(r_grad[1], r_grad[0]), neighbours(r_rim[1], r_rim[0])
    spread_gradient(2, [extended(x, edge) for x, edge in zip(inner, rim)])
    add_gradient(range(6, 9), False)

    odd = pgrad[1].reshape(BASES * ROWS, LANES)
    folded = pgrad[0].reshape(BASES * ROWS, LANES) + 0.5 * (odd + lane_roll(odd, 1))
    pg_ref[...] = folded.astype(BF16)

    for copy in started:
        copy.wait_send()


def last_product(wb_ref, pg_ref, out_ref):
    got = jnp.dot(wb_ref[...], pg_ref[...], preferred_element_type=F32)
    out_ref[...] = got[:, : out_ref.shape[2]].reshape(out_ref.shape)


def on_device(sizes, hidden_state, filter_coefficients, meridian_offset_table, function_pick_table, observation, latitude_cosine_factor):
    nx, ny, nlat = sizes
    channels, band, columns = hidden_state.shape[1:]
    hbm = pl.BlockSpec(memory_space=pltpu.HBM)
    vmem = pl.BlockSpec(memory_space=pltpu.VMEM)
    row = pltpu.VMEM((8, LANES), F32)
    sums = pltpu.VMEM((ROWS, LANES), SUMS)
    field = pltpu.VMEM((ROWS, LANES), HALO)
    edge = pltpu.VMEM((ROWS, TILE), HALO)
    raw = pltpu.VMEM((channels, band, columns), BF16)
    copies = 11 + 2 * (ny - 1) + 2 * ny * (nx - 1)
    gradient, weights = pl.pallas_call(
        functools.partial(kernel, nx, ny, nlat),
        out_shape=(
            jax.ShapeDtypeStruct((BASES * ROWS, LANES), BF16),
            jax.ShapeDtypeStruct((2 * channels, BASES * ROWS), BF16),
        ),
        in_specs=[hbm] * 7,
        out_specs=(vmem, vmem),
        scratch_shapes=[
            pltpu.SMEM((band, 3), jnp.int32),
            pltpu.SMEM((band,), F32),
            raw,
            pltpu.VMEM(filter_coefficients.shape, BF16),
            pltpu.VMEM(function_pick_table.shape, jnp.int32),
            pltpu.VMEM(observation.shape, F32),
            pltpu.VMEM((80, 18), BF16),
            pltpu.SemaphoreType.DMA((7,)),
            raw,
            pltpu.VMEM((2, 2 * channels, LANES), BF16),
            pltpu.VMEM((2 * ROWS, LANES), F32),
            pltpu.VMEM((2, 9, 3, 8, LANES), F32),
            pltpu.VMEM((2, 9, 8, LANES), F32),
            pltpu.VMEM((2, 9, 8, LANES), F32),
            pltpu.VMEM((2, 9, 3, 8, LANES), F32),
            pltpu.VMEM((2, 9, 3, 8, LANES), F32),
            pltpu.VMEM((2, 9, 3, 8, LANES), F32),
            row, row, pltpu.VMEM((2, 8, LANES), F32),
            sums, sums, pltpu.VMEM((2, ROWS, LANES), SUMS),
            pltpu.VMEM((2, 9, 8, TILE), F32),
            pltpu.VMEM((2, 9, 8, TILE), F32),
            pltpu.VMEM((40, LANES), BF16),
            pltpu.VMEM((ny - 1, 40, LANES), BF16),
            pltpu.VMEM((ny, nx - 1, 40, LANES), BF16),
            pltpu.VMEM((2, 3, 8, TILE), F32),
            pltpu.VMEM((2, 3, 8, TILE), F32),
            field, field, pltpu.VMEM((2, ROWS, LANES), HALO),
            edge, edge, pltpu.VMEM((2, ROWS, TILE), HALO),
            pltpu.SemaphoreType.DMA((copies,)),
            pltpu.SemaphoreType.DMA((copies,)),
        ],
        compiler_params=pltpu.CompilerParams(collective_id=0, has_side_effects=True, vmem_limit_bytes=16 << 20),
    )(
        *[
            pltpu.with_memory_space_constraint(array, pltpu.HBM)
            for array in (
                meridian_offset_table.T,
                latitude_cosine_factor,
                hidden_state.reshape(channels, band, columns),
                filter_coefficients,
                function_pick_table,
                observation,
                jnp.asarray(expand_picks(), BF16),
            )
        ]
    )
    out = pl.pallas_call(
        last_product,
        out_shape=jax.ShapeDtypeStruct((channels, band, columns), F32),
        in_specs=[vmem, vmem],
        out_specs=vmem,
        compiler_params=pltpu.CompilerParams(vmem_limit_bytes=16 << 20),
    )(weights, gradient)
    return out[None]


def solution(mesh):
    members = mesh.shape["ens"]
    nx = 4 if members % 4 == 0 and members > 4 else 2
    return jax.shard_map(
        functools.partial(on_device, (nx, members // nx, mesh.shape["lat"])),
        mesh=mesh,
        in_specs=(
            P("ens", None, "lat", "lon"),
            P(),
            P(None, "lat"),
            P(None, "lat", "lon"),
            P(None, "lat", "lon"),
            P("lat"),
        ),
        out_specs=P("ens", None, "lat", "lon"),
        check_vma=False,
    )
```

```python
import functools

import jax
import jax.numpy as jnp
import numpy as np
from jax import lax
from jax.experimental import pallas as pl
from jax.experimental.pallas import tpu as pltpu
from jax.sharding import PartitionSpec as P

SPAN = 4
BASES = 9
LANES = 384
TILE = 128
ROWS = 24
SMOOTH = 0.01
F32 = jnp.float32
BF16 = jnp.bfloat16
MESH = pl.DeviceIdType.MESH
HALO = BF16
DEEP = 96
PIECES = ((0, 40),)
ALONG_Y = (1, -1, 2)


def expand_picks():
    rows = np.zeros((104, 18), np.float32)
    for i in range(3):
        for sub in range(8):
            rows[8 * i + sub, 2 * (3 + i) + (sub & 1)] = 1
            rows[24 + 8 * i + sub, 2 * (6 + i) if sub & 1 else 2 * i + 1] = 1
            rows[48 + 8 * i + sub, 2 * (6 + i) + 1 if sub & 1 else 2 * i] = 1
        rows[72 + i, 2 * i] = 1
        rows[80 + i, 2 * (6 + i) + 1] = 1
        rows[88 + 3 + i, 2 * i] = 1
        rows[96 + 3 + i, 2 * (6 + i) + 1] = 1
    return rows


def iota(shape, dim):
    return lax.broadcasted_iota(jnp.int32, shape, dim)


def swapped(x):
    return jnp.where(iota(x.shape, x.ndim - 2) % 2 == 0, row_up(x), row_down(x))


def packed(pair):
    middle = jnp.where(iota((8, LANES), 0) < 4, pair[0][2], pltpu.roll(pair[1][2], 4, axis=0))
    return jnp.concatenate([pair[0][:2], middle[None], pair[1][:2]], axis=0)


def unpacked(x):
    return [x[:3], jnp.concatenate([x[3:], pltpu.roll(x[2], 4, axis=0)[None]], axis=0)]


def lane_roll(x, by):
    by %= x.shape[-1]
    return x if by == 0 else pltpu.roll(x, by, axis=x.ndim - 1)


def row_down(x):
    return pltpu.roll(x, 1, axis=x.ndim - 2)


def row_up(x):
    return pltpu.roll(x, x.shape[-2] - 1, axis=x.ndim - 2)


def smoothed_derivative(d):
    return d * lax.rsqrt(d * d + SMOOTH)


def shifted(pair, sign, steps):
    rolled = {}

    def at(parity, by):
        if (parity, by) not in rolled:
            rolled[parity, by] = lane_roll(pair[parity], -by)
        return rolled[parity, by]

    steps = jnp.broadcast_to(steps, pair[0].shape)
    out = []
    for parity in (0, 1):
        result = None
        for n in range(1, SPAN + 1):
            column = parity + sign * n
            value = at(column % 2, column // 2)
            result = value if result is None else jnp.where(steps == float(n), value, result)
        out.append(result)
    return out


def edge_of(x):
    lane = iota((*x.shape[:-1], TILE), x.ndim - 1)
    return jnp.where(lane < 64, x[..., :TILE], x[..., 2 * TILE :])


def extended(x, edge):
    lane = iota(edge.shape, edge.ndim - 1)
    last = jnp.where(
        lane < 104, x[..., 2 * TILE :], jnp.where(lane < 112, lane_roll(edge, 104), lane_roll(edge, 24))
    )
    return jnp.concatenate([x[..., : 2 * TILE], last], axis=-1)


def kernel(
    nx, ny, nlat, off_hbm, cos_hbm, x_hbm, w_hbm, pk_hbm, obs_hbm, ex_hbm, pg_ref, wb_ref,
    off_ref, cos_ref, x_raw, w_ref, pk_ref, obs_ref, ex_ref, in_sem, x_par, x_pad, x_row, x_rim, r_row, r_edge, obs_tmp,
    prod, far, qpf, qp, mask, csum, fsel, pgrad, su, sd, r_picks,
    qpe, rqpe, own, yblk, xblk, fe, rfe, f0, f1, r_grad, f0e, f1e, r_rim, send_sem, recv_sem,
):
    ens = lax.axis_index("ens")
    lat = lax.axis_index("lat")
    lon = lax.axis_index("lon")
    ex, ey = ens // ny, ens % ny
    has_up = (lat + nlat - 1) // nlat
    has_down = (2 * nlat - 2 - lat) // nlat
    partner = 1 - lon
    have_up = has_up.astype(F32)
    have_down = has_down.astype(F32)
    up = {"t": lat - has_up, "n": has_up * lon + (1 - has_up) * partner}
    down = {"t": lat + has_down, "n": has_down * lon + (1 - has_down) * partner}
    up_partner = {"t": lat - has_up, "n": partner}
    down_partner = {"t": lat + has_down, "n": partner}

    def x_peer(d):
        return ((ex + d) % nx) * ny + ey

    def y_peer(d):
        return ex * ny + (ey + d) % ny

    def target(e=None, t=None, n=None):
        return (ens if e is None else e, lat if t is None else t, lon if n is None else n)

    def step_of(a, q):
        return off_ref[q, a].astype(F32)

    sems = [0]

    def remote(src, dst, device):
        i = sems[0]
        sems[0] += 1
        return pltpu.make_async_remote_copy(
            src_ref=src, dst_ref=dst, send_sem=send_sem.at[i], recv_sem=recv_sem.at[i],
            device_id=device, device_id_type=MESH,
        )

    barrier = pltpu.get_barrier_semaphore()
    peers = [target(n=partner)]
    peers += [target(**where) for where in (up, down, up_partner, down_partner)]
    peers += [target(e=x_peer(d)) for d in range(1, nx)] + [target(e=y_peer(d)) for d in range(1, ny)]
    for device in peers:
        pl.semaphore_signal(barrier, inc=1, device_id=device, device_id_type=MESH)

    inputs = {}
    pairs = [
        ("ex", ex_hbm, ex_ref), ("pk", pk_hbm, pk_ref), ("off", off_hbm, off_ref), ("x", x_hbm, x_raw),
        ("w", w_hbm, w_ref), ("obs", obs_hbm, obs_ref), ("cos", cos_hbm, cos_ref),
    ]
    for i, (name, src, dst) in enumerate(pairs):
        inputs[name] = pltpu.make_async_copy(src, dst, in_sem.at[i])
        inputs[name].start()

    inputs["x"].wait()
    x_row[...] = jnp.zeros_like(x_row)
    for r in (0, 1):
        x_row[r, : x_raw.shape[0], : x_raw.shape[2]] = x_raw[:, r, :]
        x_rim[r] = edge_of(x_row[r].astype(F32)).astype(BF16)
    pl.semaphore_wait(barrier, len(peers))
    started = []

    def go(src, dst, device):
        copy = remote(src, dst, device)
        copy.start()
        started.append(copy)
        return copy

    def halo(to_up, to_down, into, where_up, where_down):
        base = sems[0]
        sems[0] += 2
        slots = [(to_up, where_up, has_up), (to_down, where_down, 1 - has_down)]
        arrivals = []
        for i, (src, where, slot) in enumerate(slots):
            def copy(index, src=src, where=where, i=i):
                return pltpu.make_async_remote_copy(
                    src_ref=src, dst_ref=into.at[index], send_sem=send_sem.at[base + i],
                    recv_sem=recv_sem.at[base + index], device_id=target(**where), device_id_type=MESH,
                )

            out = copy(slot)
            out.start()
            started.append(out)
            arrivals.append(copy(i))
        return arrivals

    c_rows = halo(x_row.at[0], x_row.at[1], r_row, up, down)
    c_rims = halo(x_rim.at[0], x_rim.at[1], r_edge, up_partner, down_partner)
    c_x = go(x_raw, x_par, target(n=partner))

    pick = iota((256, 256), 0) - 2 * iota((256, 256), 1)
    half = iota((256, 256), 1)
    select = jnp.where((pick == jnp.where(half < TILE, 0, -255)), 1.0, 0.0).astype(BF16)
    columns = pk_ref.shape[2]
    widths = [slice(256 * block, min(256 * block + 256, columns)) for block in range(3)]
    inputs["ex"].wait()
    inputs["pk"].wait()
    picks = pk_ref[...].astype(F32).reshape(18, columns).astype(BF16)
    rows = jnp.dot(ex_ref[...], picks, preferred_element_type=F32).astype(BF16)
    inputs["off"].wait()
    row8 = iota((8, TILE), 0)
    for block in range(3):
        wide = widths[block]
        part = select[: wide.stop - wide.start]
        tile = slice(TILE * block, TILE * block + TILE)
        got = jnp.dot(rows[:, wide], part, preferred_element_type=F32)
        for slot in range(6):
            qp[0, slot, :, tile] = got[8 * slot : 8 * slot + 8, :TILE]
            qp[1, slot, :, tile] = got[8 * slot : 8 * slot + 8, TILE:]
        for slot in range(3):
            qpf[0, slot, :, tile] = got[48 + 8 * slot : 56 + 8 * slot, :TILE]
            qpf[1, slot, :, tile] = got[48 + 8 * slot : 56 + 8 * slot, TILE:]
        su[:, tile] = jnp.where(row8 == 6, step_of(0, 0), got[72:80, :TILE] + got[88:96, TILE:])
        sd[:, tile] = jnp.where(row8 == 6, step_of(2, 1), got[80:88, :TILE] + got[96:104, TILE:])
    c_picks = halo(su, sd, r_picks, up, down)

    inputs["w"].wait()
    latents = 2 * x_raw.shape[0]
    one = jnp.where(iota((ROWS, 10), 0) // 2 == iota((ROWS, 10), 1), 1.0, 0.0).astype(BF16)
    spread = [jnp.dot(one, w_ref[k], preferred_element_type=F32) for k in range(BASES)]
    spread = jnp.concatenate(spread, axis=0).astype(BF16)
    shape = (w_ref.shape[2], latents)
    s2 = jnp.where(iota(shape, 1) // 2 == iota(shape, 0), 1.0, 0.0).astype(BF16)
    wf = jnp.dot(spread, s2, preferred_element_type=F32)
    wf = jnp.where(iota(wf.shape, 0) % 2 == iota(wf.shape, 1) % 2, wf, 0.0).astype(BF16)
    s2t = jnp.where(iota(shape[::-1], 0) // 2 == iota(shape[::-1], 1), 1.0, 0.0).astype(BF16)
    wb = lax.dot_general(s2t, spread, (((1,), (1,)), ((), ())), preferred_element_type=F32)
    wb_ref[...] = jnp.where(iota(wb.shape, 0) % 2 == iota(wb.shape, 1) % 2, wb, 0.0).astype(BF16)
    shape = (w_ref.shape[2], 2 * DEEP)
    s3 = jnp.where(iota(shape, 1) % DEEP == iota(shape, 0), 1.0, 0.0).astype(BF16)
    wn = jnp.dot(spread, s3, preferred_element_type=F32)
    wn = jnp.where((iota(wn.shape, 0) % 2 == 0) == (iota(wn.shape, 1) < DEEP), wn, 0.0).astype(BF16)

    inputs["obs"].wait()
    obs = obs_ref[...].reshape(20, columns)
    obs_hi = obs.astype(BF16)
    obs_lo = (obs - obs_hi.astype(F32)).astype(BF16)
    obs_tmp[...] = jnp.zeros_like(obs_tmp)
    for block in range(3):
        wide = widths[block]
        part = select[: wide.stop - wide.start]
        tile = slice(TILE * block, TILE * block + TILE)
        both = jnp.dot(obs_hi[:, wide], part, preferred_element_type=F32) + jnp.dot(
            obs_lo[:, wide], part, preferred_element_type=F32
        )
        obs_tmp[: obs.shape[0], tile] = both[:, :TILE]
        obs_tmp[ROWS : ROWS + obs.shape[0], tile] = both[:, TILE:]
    inputs["cos"].wait()

    c_x.wait_recv()
    sector = []
    for i, raw in enumerate((x_raw, x_par)):
        x_pad[i, :, 2 * TILE :] = jnp.zeros((latents, TILE), BF16)
        x_pad[i, :, : columns // 2] = raw[...].reshape(latents, columns // 2)
        sector.append(x_pad[i].astype(F32))
    latent = extended(sector[0], edge_of(sector[1]))
    halfway = 0.5 * (latent + lane_roll(latent, -1))
    for parity, x in enumerate((latent, halfway)):
        got = jnp.dot(wf, x.astype(BF16), preferred_element_type=F32)
        prod[parity] = got.reshape(BASES, 3, 8, LANES)

    even = iota((8, LANES), 0) % 2 == 0
    even3 = iota((3, 8, LANES), 1) % 2 == 0
    steps = [
        jnp.where(even, step_of(1, 0), step_of(1, 1)),
        jnp.where(even, step_of(0, 1), step_of(2, 0)),
        jnp.where(even, step_of(0, 0), step_of(2, 1)),
    ]

    def build_masks(kind, source):
        for b in (-1, 0, 1):
            slot = 3 * kind + b + 1
            pair = source(slot)
            if b:
                pair = shifted(pair, -b, steps[kind])
            for parity in (0, 1):
                mask[parity, slot] = pair[parity]

    def own_columns(slot):
        return [qp[0, slot], qp[1, slot]]

    def all_columns(slot):
        return [extended(qp[parity, slot], rqpe[parity, slot]) for parity in (0, 1)]

    def pick_products(product, slots):
        for parity in (0, 1):
            for t in range(3):
                tile = slice(TILE * t, TILE * t + TILE)
                values = [product[parity, k, :, :, tile] for k in range(BASES)]
                for slot in slots:
                    want = jnp.broadcast_to(mask[parity, slot, :, tile][None], (3, 8, TILE))
                    total = jnp.where(want == 0.0, values[0], 0.0)
                    for k in range(1, BASES):
                        total = jnp.where(want == float(k), values[k], total)
                    csum[parity, slot, :, :, tile] = total

    def target_sum(kind):
        total = [csum[0, 3 * kind + 1], csum[1, 3 * kind + 1]]
        for b in (-1, 1):
            slot = 3 * kind + b + 1
            moved = shifted([csum[0, slot], csum[1, slot]], b, steps[kind])
            total = [x + y for x, y in zip(total, moved)]
        return total

    for kind in (0, 1):
        build_masks(kind, own_columns)
    pick_products(prod, range(6))
    local = [x + swapped(y) for x, y in zip(target_sum(0), target_sum(1))]
    build_masks(2, lambda slot: [qpf[0, slot - 6], qpf[1, slot - 6]])

    for copy in c_rows + c_rims:
        copy.wait_recv()
    around_x = extended(
        r_row[...].reshape(2 * DEEP, LANES).astype(F32), r_edge[...].reshape(2 * DEEP, TILE).astype(F32)
    )
    for parity, x in enumerate((around_x, 0.5 * (around_x + lane_roll(around_x, -1)))):
        far[parity] = jnp.dot(wn, x.astype(BF16), preferred_element_type=F32).reshape(BASES, 3, 8, LANES)
    pick_products(far, range(6, 9))
    present = jnp.where(even3, have_up, have_down)
    pred = [x + present * y for x, y in zip(local, target_sum(2))]
    mine = packed(pred)
    own[...] = mine.reshape(40, LANES).astype(BF16)

    def spread_row(i):
        return jnp.where(
            even,
            jnp.broadcast_to(r_picks[0, i : i + 1, :], (8, LANES)),
            jnp.broadcast_to(r_picks[1, i : i + 1, :], (8, LANES)),
        )

    def backward_masks():
        for copy in c_picks:
            copy.wait_recv()
        steps[2] = spread_row(6)
        for parity in (0, 1):
            for i in range(3):
                qp[parity, 6 + i] = spread_row(3 * parity + i)
            qpe[parity] = edge_of(qp[parity])
        go(qpe, rqpe, target(n=partner)).wait_recv()
        for kind in range(3):
            build_masks(kind, all_columns)

    def terms(ref):
        return smoothed_derivative(mine - ref[...].astype(F32).reshape(5, 8, LANES))

    if nx == 4:
        ring = (1, -1, 2)

        def slot(dx, dy, rows):
            place = xblk.at[ring.index(dy) + 1 if dy else 0, ring.index(dx)] if dx else yblk.at[ring.index(dy)]
            return place.at[pl.ds(*rows)]

        arrivals = {}
        for rows in PIECES:
            for dy in ALONG_Y:
                arrivals[0, dy, rows] = go(own.at[pl.ds(*rows)], slot(0, dy, rows), target(e=y_peer(dy % ny)))
        for rows in PIECES:
            for dx in ring:
                arrivals[dx, 0, rows] = go(own.at[pl.ds(*rows)], slot(dx, 0, rows), target(e=x_peer(dx % nx)))
        backward_masks()
        for rows in PIECES:
            for dy in ring:
                arrivals[0, dy, rows].wait_recv()
                for dx in ring:
                    arrivals[dx, dy, rows] = go(slot(0, dy, rows), slot(dx, dy, rows), target(e=x_peer(dx % nx)))
        pair_total = jnp.zeros_like(mine)
        for dy in (0, *ring):
            if dy:
                pair_total += terms(yblk.at[ring.index(dy)])
            for dx in ring:
                for rows in PIECES:
                    arrivals[dx, dy, rows].wait_recv()
                pair_total += terms(xblk.at[ring.index(dy) + 1 if dy else 0, ring.index(dx)])
    else:
        c_y = [go(own, yblk.at[d - 1], target(e=y_peer(d))) for d in range(1, ny)]
        relayed = [[go(own, xblk.at[0, d - 1], target(e=x_peer(d))) for d in range(1, nx)]]
        pair_total = jnp.zeros_like(mine)
        for d in range(1, ny):
            c_y[d - 1].wait_recv()
            relayed.append([go(yblk.at[d - 1], xblk.at[d, e - 1], target(e=x_peer(e))) for e in range(1, nx)])
            pair_total += terms(yblk.at[d - 1])
        backward_masks()
        for d in range(ny):
            for e in range(1, nx):
                relayed[d][e - 1].wait_recv()
                pair_total += terms(xblk.at[d, e - 1])
    pair_total = unpacked(pair_total)

    factor = jnp.where(even3, cos_ref[0], cos_ref[1])
    grad = []
    for parity in (0, 1):
        miss = pred[parity] - obs_tmp[ROWS * parity : ROWS * (parity + 1)].reshape(3, 8, LANES)
        grad.append(factor * (smoothed_derivative(miss) - pair_total[parity] * (1.0 / (nx * ny - 1))))
        fe[parity] = edge_of(grad[parity])
    lower = jnp.where(even3, grad[0], row_down(grad[1]))
    upper = jnp.where(even3, row_up(grad[0]), grad[1])
    f0[...] = lower.reshape(ROWS, LANES).astype(f0.dtype)
    f1[...] = upper.reshape(ROWS, LANES).astype(f1.dtype)
    f0e[...] = edge_of(lower).reshape(ROWS, TILE).astype(f0e.dtype)
    f1e[...] = edge_of(upper).reshape(ROWS, TILE).astype(f1e.dtype)
    c_fe = go(fe, rfe, target(n=partner))
    c_f = halo(f0, f1, r_grad, up, down) + halo(f0e, f1e, r_rim, up_partner, down_partner)

    def spread_gradient(kind, wide):
        for b in (-1, 0, 1):
            pair = shifted(wide, -b, steps[kind]) if b else wide
            for parity in (0, 1):
                fsel[parity, 3 * kind + b + 1] = pair[parity]

    def add_gradient(slots, first):
        for parity in (0, 1):
            for t in range(3):
                tile = slice(TILE * t, TILE * t + TILE)
                values = [fsel[parity, slot, :, :, tile] for slot in slots]
                wants = [jnp.broadcast_to(mask[parity, slot, :, tile][None], (3, 8, TILE)) for slot in slots]
                for k in range(BASES):
                    chosen = [jnp.where(want == float(k), value, 0.0) for want, value in zip(wants, values)]
                    if not first:
                        chosen.append(pgrad[parity, k, :, :, tile])
                    while len(chosen) > 1:
                        chosen = [x + y for x, y in zip(chosen[::2], chosen[1::2])] + chosen[len(chosen) & ~1 :]
                    pgrad[parity, k, :, :, tile] = chosen[0]

    c_fe.wait_recv()
    wide = [extended(grad[parity], rfe[parity]) for parity in (0, 1)]
    spread_gradient(0, wide)
    spread_gradient(1, [swapped(x) for x in wide])
    add_gradient(range(6), True)

    def neighbours(below, above):
        below = below.astype(F32).reshape(3, 8, -1) * have_down
        above = above.astype(F32).reshape(3, 8, -1) * have_up
        is_even = iota(below.shape, 1) % 2 == 0
        return [jnp.where(is_even, above, row_down(below)), jnp.where(is_even, row_up(above), below)]

    for copy in c_f:
        copy.wait_recv()
    inner, rim = neighbours(r_grad[1], r_grad[0]), neighbours(r_rim[1], r_rim[0])
    spread_gradient(2, [extended(x, edge) for x, edge in zip(inner, rim)])
    add_gradient(range(6, 9), False)

    odd = pgrad[1].reshape(BASES * ROWS, LANES)
    folded = pgrad[0].reshape(BASES * ROWS, LANES) + 0.5 * (odd + lane_roll(odd, 1))
    pg_ref[...] = folded.astype(BF16)

    for copy in started:
        copy.wait_send()


def last_product(wb_ref, pg_ref, out_ref):
    got = jnp.dot(wb_ref[...], pg_ref[...], preferred_element_type=F32)
    out_ref[...] = got[:, : out_ref.shape[2]].reshape(out_ref.shape)


def on_device(sizes, hidden_state, filter_coefficients, meridian_offset_table, function_pick_table, observation, latitude_cosine_factor):
    nx, ny, nlat = sizes
    channels, band, columns = hidden_state.shape[1:]
    hbm = pl.BlockSpec(memory_space=pltpu.HBM)
    vmem = pl.BlockSpec(memory_space=pltpu.VMEM)
    row = pltpu.VMEM((8, LANES), F32)
    field = pltpu.VMEM((ROWS, LANES), HALO)
    edge = pltpu.VMEM((ROWS, TILE), HALO)
    raw = pltpu.VMEM((channels, band, columns), BF16)
    copies = 11 + 2 * (ny - 1) + 2 * ny * (nx - 1)
    gradient, weights = pl.pallas_call(
        functools.partial(kernel, nx, ny, nlat),
        out_shape=(
            jax.ShapeDtypeStruct((BASES * ROWS, LANES), BF16),
            jax.ShapeDtypeStruct((2 * channels, BASES * ROWS), BF16),
        ),
        in_specs=[hbm] * 7,
        out_specs=(vmem, vmem),
        scratch_shapes=[
            pltpu.SMEM((band, 3), jnp.int32),
            pltpu.SMEM((band,), F32),
            raw,
            pltpu.VMEM(filter_coefficients.shape, BF16),
            pltpu.VMEM(function_pick_table.shape, jnp.int32),
            pltpu.VMEM(observation.shape, F32),
            pltpu.VMEM((104, 18), BF16),
            pltpu.SemaphoreType.DMA((7,)),
            raw,
            pltpu.VMEM((2, 2 * channels, LANES), BF16),
            pltpu.VMEM((2, DEEP, LANES), BF16),
            pltpu.VMEM((2, DEEP, TILE), BF16),
            pltpu.VMEM((2, DEEP, LANES), BF16),
            pltpu.VMEM((2, DEEP, TILE), BF16),
            pltpu.VMEM((2 * ROWS, LANES), F32),
            pltpu.VMEM((2, 9, 3, 8, LANES), F32),
            pltpu.VMEM((2, 9, 3, 8, LANES), F32),
            pltpu.VMEM((2, 3, 8, LANES), F32),
            pltpu.VMEM((2, 9, 8, LANES), F32),
            pltpu.VMEM((2, 9, 8, LANES), F32),
            pltpu.VMEM((2, 9, 3, 8, LANES), F32),
            pltpu.VMEM((2, 9, 3, 8, LANES), F32),
            pltpu.VMEM((2, 9, 3, 8, LANES), F32),
            row, row, pltpu.VMEM((2, 8, LANES), F32),
            pltpu.VMEM((2, 9, 8, TILE), F32),
            pltpu.VMEM((2, 9, 8, TILE), F32),
            pltpu.VMEM((40, LANES), BF16),
            pltpu.VMEM((ny - 1, 40, LANES), BF16),
            pltpu.VMEM((ny, nx - 1, 40, LANES), BF16),
            pltpu.VMEM((2, 3, 8, TILE), F32),
            pltpu.VMEM((2, 3, 8, TILE), F32),
            field, field, pltpu.VMEM((2, ROWS, LANES), HALO),
            edge, edge, pltpu.VMEM((2, ROWS, TILE), HALO),
            pltpu.SemaphoreType.DMA((copies,)),
            pltpu.SemaphoreType.DMA((copies,)),
        ],
        compiler_params=pltpu.CompilerParams(collective_id=0, has_side_effects=True, vmem_limit_bytes=16 << 20),
    )(
        *[
            pltpu.with_memory_space_constraint(array, pltpu.HBM)
            for array in (
                meridian_offset_table.T,
                latitude_cosine_factor,
                hidden_state.reshape(channels, band, columns),
                filter_coefficients,
                function_pick_table,
                observation,
                jnp.asarray(expand_picks(), BF16),
            )
        ]
    )
    out = pl.pallas_call(
        last_product,
        out_shape=jax.ShapeDtypeStruct((channels, band, columns), F32),
        in_specs=[vmem, vmem],
        out_specs=vmem,
        compiler_params=pltpu.CompilerParams(vmem_limit_bytes=16 << 20),
    )(weights, gradient)
    return out[None]


def solution(mesh):
    members = mesh.shape["ens"]
    nx = 4 if members % 4 == 0 and members > 4 else 2
    return jax.shard_map(
        functools.partial(on_device, (nx, members // nx, mesh.shape["lat"])),
        mesh=mesh,
        in_specs=(
            P("ens", None, "lat", "lon"),
            P(),
            P(None, "lat"),
            P(None, "lat", "lon"),
            P(None, "lat", "lon"),
            P("lat"),
        ),
        out_specs=P("ens", None, "lat", "lon"),
        check_vma=False,
    )
```

```python
import functools

import jax
import jax.numpy as jnp
import numpy as np
from jax import lax
from jax.experimental import pallas as pl
from jax.experimental.pallas import tpu as pltpu
from jax.sharding import PartitionSpec as P

SPAN = 4
BASES = 9
LANES = 384
TILE = 128
ROWS = 24
SMOOTH = 0.01
F32 = jnp.float32
BF16 = jnp.bfloat16
MESH = pl.DeviceIdType.MESH
HALO = BF16
DEEP = 96
PIECES = ((0, 40),)
ALONG_Y = (1, -1, 2)


def expand_picks():
    rows = np.zeros((104, 18), np.float32)
    for i in range(3):
        for sub in range(8):
            rows[8 * i + sub, 2 * (3 + i) + (sub & 1)] = 1
            rows[24 + 8 * i + sub, 2 * (6 + i) if sub & 1 else 2 * i + 1] = 1
            rows[48 + 8 * i + sub, 2 * (6 + i) + 1 if sub & 1 else 2 * i] = 1
        rows[72 + i, 2 * i] = 1
        rows[80 + i, 2 * (6 + i) + 1] = 1
        rows[88 + 3 + i, 2 * i] = 1
        rows[96 + 3 + i, 2 * (6 + i) + 1] = 1
    return rows


def iota(shape, dim):
    return lax.broadcasted_iota(jnp.int32, shape, dim)


def swapped(x):
    return jnp.where(iota(x.shape, x.ndim - 2) % 2 == 0, row_up(x), row_down(x))


def packed(pair):
    middle = jnp.where(iota((8, LANES), 0) < 4, pair[0][2], pltpu.roll(pair[1][2], 4, axis=0))
    return jnp.concatenate([pair[0][:2], middle[None], pair[1][:2]], axis=0)


def unpacked(x):
    return [x[:3], jnp.concatenate([x[3:], pltpu.roll(x[2], 4, axis=0)[None]], axis=0)]


def lane_roll(x, by):
    by %= x.shape[-1]
    return x if by == 0 else pltpu.roll(x, by, axis=x.ndim - 1)


def row_down(x):
    return pltpu.roll(x, 1, axis=x.ndim - 2)


def row_up(x):
    return pltpu.roll(x, x.shape[-2] - 1, axis=x.ndim - 2)


def smoothed_derivative(d):
    return d * lax.rsqrt(d * d + SMOOTH)


def shifted(pair, sign, steps):
    rolled = {}

    def at(parity, by):
        if (parity, by) not in rolled:
            rolled[parity, by] = lane_roll(pair[parity], -by)
        return rolled[parity, by]

    steps = jnp.broadcast_to(steps, pair[0].shape)
    out = []
    for parity in (0, 1):
        result = None
        for n in range(1, SPAN + 1):
            column = parity + sign * n
            value = at(column % 2, column // 2)
            result = value if result is None else jnp.where(steps == float(n), value, result)
        out.append(result)
    return out


def edge_of(x):
    lane = iota((*x.shape[:-1], TILE), x.ndim - 1)
    return jnp.where(lane < 64, x[..., :TILE], x[..., 2 * TILE :])


def extended(x, edge):
    lane = iota(edge.shape, edge.ndim - 1)
    last = jnp.where(
        lane < 104, x[..., 2 * TILE :], jnp.where(lane < 112, lane_roll(edge, 104), lane_roll(edge, 24))
    )
    return jnp.concatenate([x[..., : 2 * TILE], last], axis=-1)


def kernel(
    nx, ny, nlat, off_hbm, cos_hbm, x_hbm, w_hbm, pk_hbm, obs_hbm, ex_hbm, pg_ref, wb_ref,
    off_ref, cos_ref, x_raw, w_ref, pk_ref, obs_ref, ex_ref, in_sem, x_par, x_pad, x_row, x_rim, r_row, r_edge, obs_tmp,
    prod, far, qpf, qp, mask, csum, fsel, pgrad, su, sd, r_picks,
    qpe, rqpe, own, yblk, xblk, fe, rfe, f0, f1, r_grad, f0e, f1e, r_rim, ring_sem, send_sem, recv_sem,
):
    ens = lax.axis_index("ens")
    lat = lax.axis_index("lat")
    lon = lax.axis_index("lon")
    ex, ey = ens // ny, ens % ny
    has_up = (lat + nlat - 1) // nlat
    has_down = (2 * nlat - 2 - lat) // nlat
    partner = 1 - lon
    have_up = has_up.astype(F32)
    have_down = has_down.astype(F32)
    up = {"t": lat - has_up, "n": has_up * lon + (1 - has_up) * partner}
    down = {"t": lat + has_down, "n": has_down * lon + (1 - has_down) * partner}
    up_partner = {"t": lat - has_up, "n": partner}
    down_partner = {"t": lat + has_down, "n": partner}

    def x_peer(d):
        return ((ex + d) % nx) * ny + ey

    def y_peer(d):
        return ex * ny + (ey + d) % ny

    def target(e=None, t=None, n=None):
        return (ens if e is None else e, lat if t is None else t, lon if n is None else n)

    def step_of(a, q):
        return off_ref[q, a].astype(F32)

    sems = [0]

    def remote(src, dst, device):
        i = sems[0]
        sems[0] += 1
        return pltpu.make_async_remote_copy(
            src_ref=src, dst_ref=dst, send_sem=send_sem.at[i], recv_sem=recv_sem.at[i],
            device_id=device, device_id_type=MESH,
        )

    inputs = {}
    pairs = [
        ("x", x_hbm, x_raw), ("ex", ex_hbm, ex_ref), ("pk", pk_hbm, pk_ref), ("off", off_hbm, off_ref),
        ("w", w_hbm, w_ref), ("obs", obs_hbm, obs_ref), ("cos", cos_hbm, cos_ref),
    ]
    for i, (name, src, dst) in enumerate(pairs):
        inputs[name] = pltpu.make_async_copy(src, dst, in_sem.at[i])
        inputs[name].start()

    barrier = pltpu.get_barrier_semaphore()
    peers = [target(n=partner)]
    peers += [target(**where) for where in (up, down, up_partner, down_partner)]
    peers += [target(e=x_peer(d)) for d in (1, nx - 1)[: nx - 1]] + [target(e=y_peer(d)) for d in (1, ny - 1)[: ny - 1]]
    for device in peers:
        pl.semaphore_signal(barrier, inc=1, device_id=device, device_id_type=MESH)

    channels, latent_columns = x_raw.shape[0], x_raw.shape[2]
    latents = 2 * channels
    shape = (2 * DEEP, latents)
    wanted = jnp.where(iota(shape, 0) < DEEP, 2 * iota(shape, 0), 2 * (iota(shape, 0) - DEEP) + 1)
    wanted = jnp.where(wanted == iota(shape, 1), 1.0, 0.0).astype(BF16)
    for i in (0, 1):
        x_pad[i, :, 2 * TILE :] = jnp.zeros((latents, TILE), BF16)
    inputs["x"].wait()
    x_pad[0, :, :latent_columns] = x_raw[...].reshape(latents, latent_columns)
    split = jnp.dot(wanted, x_pad[0], preferred_element_type=F32)
    for r in (0, 1):
        row = split[DEEP * r : DEEP * (r + 1)]
        x_row[r] = row.astype(BF16)
        x_rim[r] = edge_of(row).astype(BF16)
    pl.semaphore_wait(barrier, len(peers))
    started = []

    def go(src, dst, device):
        copy = remote(src, dst, device)
        copy.start()
        started.append(copy)
        return copy

    def halo(to_up, to_down, into, where_up, where_down):
        base = sems[0]
        sems[0] += 2
        slots = [(to_up, where_up, has_up), (to_down, where_down, 1 - has_down)]
        arrivals = []
        for i, (src, where, slot) in enumerate(slots):
            def copy(index, src=src, where=where, i=i):
                return pltpu.make_async_remote_copy(
                    src_ref=src, dst_ref=into.at[index], send_sem=send_sem.at[base + i],
                    recv_sem=recv_sem.at[base + index], device_id=target(**where), device_id_type=MESH,
                )

            out = copy(slot)
            out.start()
            started.append(out)
            arrivals.append(copy(i))
        return arrivals

    if nx == 4:
        for device in (target(e=x_peer(1)), target(e=y_peer(1))):
            pl.semaphore_signal(ring_sem, inc=1, device_id=device, device_id_type=MESH)
    c_rows = halo(x_row.at[0], x_row.at[1], r_row, up, down)
    c_rims = halo(x_rim.at[0], x_rim.at[1], r_edge, up_partner, down_partner)
    c_x = go(x_raw, x_par, target(n=partner))

    pick = iota((256, 256), 0) - 2 * iota((256, 256), 1)
    half = iota((256, 256), 1)
    select = jnp.where((pick == jnp.where(half < TILE, 0, -255)), 1.0, 0.0).astype(BF16)
    columns = pk_ref.shape[2]
    widths = [slice(256 * block, min(256 * block + 256, columns)) for block in range(3)]
    inputs["ex"].wait()
    inputs["pk"].wait()
    picks = pk_ref[...].astype(F32).reshape(18, columns).astype(BF16)
    rows = jnp.dot(ex_ref[...], picks, preferred_element_type=F32).astype(BF16)
    inputs["off"].wait()
    row8 = iota((8, TILE), 0)
    for block in range(3):
        wide = widths[block]
        part = select[: wide.stop - wide.start]
        tile = slice(TILE * block, TILE * block + TILE)
        got = jnp.dot(rows[:, wide], part, preferred_element_type=F32)
        for slot in range(6):
            qp[0, slot, :, tile] = got[8 * slot : 8 * slot + 8, :TILE]
            qp[1, slot, :, tile] = got[8 * slot : 8 * slot + 8, TILE:]
        for slot in range(3):
            qpf[0, slot, :, tile] = got[48 + 8 * slot : 56 + 8 * slot, :TILE]
            qpf[1, slot, :, tile] = got[48 + 8 * slot : 56 + 8 * slot, TILE:]
        su[:, tile] = jnp.where(row8 == 6, step_of(0, 0), got[72:80, :TILE] + got[88:96, TILE:])
        sd[:, tile] = jnp.where(row8 == 6, step_of(2, 1), got[80:88, :TILE] + got[96:104, TILE:])
    c_picks = halo(su, sd, r_picks, up, down)

    inputs["w"].wait()
    one = jnp.where(iota((ROWS, 10), 0) // 2 == iota((ROWS, 10), 1), 1.0, 0.0).astype(BF16)
    spread = [jnp.dot(one, w_ref[k], preferred_element_type=F32) for k in range(BASES)]
    spread = jnp.concatenate(spread, axis=0).astype(BF16)
    shape = (w_ref.shape[2], latents)
    s2 = jnp.where(iota(shape, 1) // 2 == iota(shape, 0), 1.0, 0.0).astype(BF16)
    wf = jnp.dot(spread, s2, preferred_element_type=F32)
    wf = jnp.where(iota(wf.shape, 0) % 2 == iota(wf.shape, 1) % 2, wf, 0.0).astype(BF16)
    s2t = jnp.where(iota(shape[::-1], 0) // 2 == iota(shape[::-1], 1), 1.0, 0.0).astype(BF16)
    wb = lax.dot_general(s2t, spread, (((1,), (1,)), ((), ())), preferred_element_type=F32)
    wb_ref[...] = jnp.where(iota(wb.shape, 0) % 2 == iota(wb.shape, 1) % 2, wb, 0.0).astype(BF16)
    shape = (w_ref.shape[2], 2 * DEEP)
    s3 = jnp.where(iota(shape, 1) % DEEP == iota(shape, 0), 1.0, 0.0).astype(BF16)
    wn = jnp.dot(spread, s3, preferred_element_type=F32)
    wn = jnp.where((iota(wn.shape, 0) % 2 == 0) == (iota(wn.shape, 1) < DEEP), wn, 0.0).astype(BF16)

    inputs["obs"].wait()
    obs = obs_ref[...].reshape(20, columns)
    obs_hi = obs.astype(BF16)
    obs_lo = (obs - obs_hi.astype(F32)).astype(BF16)
    obs_tmp[...] = jnp.zeros_like(obs_tmp)
    for block in range(3):
        wide = widths[block]
        part = select[: wide.stop - wide.start]
        tile = slice(TILE * block, TILE * block + TILE)
        both = jnp.dot(obs_hi[:, wide], part, preferred_element_type=F32) + jnp.dot(
            obs_lo[:, wide], part, preferred_element_type=F32
        )
        obs_tmp[: obs.shape[0], tile] = both[:, :TILE]
        obs_tmp[ROWS : ROWS + obs.shape[0], tile] = both[:, TILE:]
    inputs["cos"].wait()

    c_x.wait_recv()
    x_pad[1, :, :latent_columns] = x_par[...].reshape(latents, latent_columns)
    sector = [x_pad[i].astype(F32) for i in (0, 1)]
    latent = extended(sector[0], edge_of(sector[1]))
    halfway = 0.5 * (latent + lane_roll(latent, -1))
    for parity, x in enumerate((latent, halfway)):
        got = jnp.dot(wf, x.astype(BF16), preferred_element_type=F32)
        prod[parity] = got.reshape(BASES, 3, 8, LANES)

    even = iota((8, LANES), 0) % 2 == 0
    even3 = iota((3, 8, LANES), 1) % 2 == 0
    steps = [
        jnp.where(even, step_of(1, 0), step_of(1, 1)),
        jnp.where(even, step_of(0, 1), step_of(2, 0)),
        jnp.where(even, step_of(0, 0), step_of(2, 1)),
    ]

    def build_masks(kind, source):
        for b in (-1, 0, 1):
            slot = 3 * kind + b + 1
            pair = source(slot)
            if b:
                pair = shifted(pair, -b, steps[kind])
            for parity in (0, 1):
                mask[parity, slot] = pair[parity]

    def own_columns(slot):
        return [qp[0, slot], qp[1, slot]]

    def all_columns(slot):
        return [extended(qp[parity, slot], rqpe[parity, slot]) for parity in (0, 1)]

    def pick_products(product, slots):
        for parity in (0, 1):
            for t in range(3):
                tile = slice(TILE * t, TILE * t + TILE)
                values = [product[parity, k, :, :, tile] for k in range(BASES)]
                for slot in slots:
                    want = jnp.broadcast_to(mask[parity, slot, :, tile][None], (3, 8, TILE))
                    total = jnp.where(want == 0.0, values[0], 0.0)
                    for k in range(1, BASES):
                        total = jnp.where(want == float(k), values[k], total)
                    csum[parity, slot, :, :, tile] = total

    def target_sum(kind):
        total = [csum[0, 3 * kind + 1], csum[1, 3 * kind + 1]]
        for b in (-1, 1):
            slot = 3 * kind + b + 1
            moved = shifted([csum[0, slot], csum[1, slot]], b, steps[kind])
            total = [x + y for x, y in zip(total, moved)]
        return total

    for kind in (0, 1):
        build_masks(kind, own_columns)
    pick_products(prod, range(6))
    local = [x + swapped(y) for x, y in zip(target_sum(0), target_sum(1))]
    build_masks(2, lambda slot: [qpf[0, slot - 6], qpf[1, slot - 6]])

    for copy in c_rows + c_rims:
        copy.wait_recv()
    around_x = extended(
        r_row[...].reshape(2 * DEEP, LANES).astype(F32), r_edge[...].reshape(2 * DEEP, TILE).astype(F32)
    )
    for parity, x in enumerate((around_x, 0.5 * (around_x + lane_roll(around_x, -1)))):
        far[parity] = jnp.dot(wn, x.astype(BF16), preferred_element_type=F32).reshape(BASES, 3, 8, LANES)
    pick_products(far, range(6, 9))
    present = jnp.where(even3, have_up, have_down)
    pred = [x + present * y for x, y in zip(local, target_sum(2))]
    mine = packed(pred)
    own[...] = mine.reshape(40, LANES).astype(BF16)

    def spread_row(i):
        return jnp.where(
            even,
            jnp.broadcast_to(r_picks[0, i : i + 1, :], (8, LANES)),
            jnp.broadcast_to(r_picks[1, i : i + 1, :], (8, LANES)),
        )

    def backward_masks():
        for copy in c_picks:
            copy.wait_recv()
        steps[2] = spread_row(6)
        for parity in (0, 1):
            for i in range(3):
                qp[parity, 6 + i] = spread_row(3 * parity + i)
            qpe[parity] = edge_of(qp[parity])
        go(qpe, rqpe, target(n=partner)).wait_recv()
        for kind in range(3):
            build_masks(kind, all_columns)

    def terms(ref):
        return smoothed_derivative(mine - ref[...].astype(F32).reshape(5, 8, LANES))

    if nx == 4:
        ring = (1, -1, 2)

        def slot(dx, dy, rows):
            place = xblk.at[ring.index(dy) + 1 if dy else 0, ring.index(dx)] if dx else yblk.at[ring.index(dy)]
            return place.at[pl.ds(*rows)]

        pl.semaphore_wait(ring_sem, 2)
        arrivals = {}
        for rows in PIECES:
            for dy in ALONG_Y:
                arrivals[0, dy, rows] = go(own.at[pl.ds(*rows)], slot(0, dy, rows), target(e=y_peer(dy % ny)))
        for rows in PIECES:
            for dx in ring:
                arrivals[dx, 0, rows] = go(own.at[pl.ds(*rows)], slot(dx, 0, rows), target(e=x_peer(dx % nx)))
        backward_masks()
        for rows in PIECES:
            for dy in ring:
                arrivals[0, dy, rows].wait_recv()
                for dx in ring:
                    arrivals[dx, dy, rows] = go(slot(0, dy, rows), slot(dx, dy, rows), target(e=x_peer(dx % nx)))
        pair_total = jnp.zeros_like(mine)
        for dy in (0, *ring):
            if dy:
                pair_total += terms(yblk.at[ring.index(dy)])
            for dx in ring:
                for rows in PIECES:
                    arrivals[dx, dy, rows].wait_recv()
                pair_total += terms(xblk.at[ring.index(dy) + 1 if dy else 0, ring.index(dx)])
    else:
        c_y = [go(own, yblk.at[d - 1], target(e=y_peer(d))) for d in range(1, ny)]
        relayed = [[go(own, xblk.at[0, d - 1], target(e=x_peer(d))) for d in range(1, nx)]]
        pair_total = jnp.zeros_like(mine)
        for d in range(1, ny):
            c_y[d - 1].wait_recv()
            relayed.append([go(yblk.at[d - 1], xblk.at[d, e - 1], target(e=x_peer(e))) for e in range(1, nx)])
            pair_total += terms(yblk.at[d - 1])
        backward_masks()
        for d in range(ny):
            for e in range(1, nx):
                relayed[d][e - 1].wait_recv()
                pair_total += terms(xblk.at[d, e - 1])
    pair_total = unpacked(pair_total)

    factor = jnp.where(even3, cos_ref[0], cos_ref[1])
    grad = []
    for parity in (0, 1):
        miss = pred[parity] - obs_tmp[ROWS * parity : ROWS * (parity + 1)].reshape(3, 8, LANES)
        grad.append(factor * (smoothed_derivative(miss) - pair_total[parity] * (1.0 / (nx * ny - 1))))
        fe[parity] = edge_of(grad[parity])
    lower = jnp.where(even3, grad[0], row_down(grad[1]))
    upper = jnp.where(even3, row_up(grad[0]), grad[1])
    f0[...] = lower.reshape(ROWS, LANES).astype(f0.dtype)
    f1[...] = upper.reshape(ROWS, LANES).astype(f1.dtype)
    f0e[...] = edge_of(lower).reshape(ROWS, TILE).astype(f0e.dtype)
    f1e[...] = edge_of(upper).reshape(ROWS, TILE).astype(f1e.dtype)
    c_fe = go(fe, rfe, target(n=partner))
    c_f = halo(f0, f1, r_grad, up, down) + halo(f0e, f1e, r_rim, up_partner, down_partner)

    def spread_gradient(kind, wide):
        for b in (-1, 0, 1):
            pair = shifted(wide, -b, steps[kind]) if b else wide
            for parity in (0, 1):
                fsel[parity, 3 * kind + b + 1] = pair[parity]

    def add_gradient(slots, first):
        for parity in (0, 1):
            for t in range(3):
                tile = slice(TILE * t, TILE * t + TILE)
                values = [fsel[parity, slot, :, :, tile] for slot in slots]
                wants = [jnp.broadcast_to(mask[parity, slot, :, tile][None], (3, 8, TILE)) for slot in slots]
                for k in range(BASES):
                    chosen = [jnp.where(want == float(k), value, 0.0) for want, value in zip(wants, values)]
                    if not first:
                        chosen.append(pgrad[parity, k, :, :, tile])
                    while len(chosen) > 1:
                        chosen = [x + y for x, y in zip(chosen[::2], chosen[1::2])] + chosen[len(chosen) & ~1 :]
                    pgrad[parity, k, :, :, tile] = chosen[0]

    c_fe.wait_recv()
    wide = [extended(grad[parity], rfe[parity]) for parity in (0, 1)]
    spread_gradient(0, wide)
    spread_gradient(1, [swapped(x) for x in wide])
    add_gradient(range(6), True)

    def neighbours(below, above):
        below = below.astype(F32).reshape(3, 8, -1) * have_down
        above = above.astype(F32).reshape(3, 8, -1) * have_up
        is_even = iota(below.shape, 1) % 2 == 0
        return [jnp.where(is_even, above, row_down(below)), jnp.where(is_even, row_up(above), below)]

    for copy in c_f:
        copy.wait_recv()
    inner, rim = neighbours(r_grad[1], r_grad[0]), neighbours(r_rim[1], r_rim[0])
    spread_gradient(2, [extended(x, edge) for x, edge in zip(inner, rim)])
    add_gradient(range(6, 9), False)

    odd = pgrad[1].reshape(BASES * ROWS, LANES)
    folded = pgrad[0].reshape(BASES * ROWS, LANES) + 0.5 * (odd + lane_roll(odd, 1))
    pg_ref[...] = folded.astype(BF16)

    for copy in started:
        copy.wait_send()


def last_product(wb_ref, pg_ref, out_ref):
    got = jnp.dot(wb_ref[...], pg_ref[...], preferred_element_type=F32)
    out_ref[...] = got[:, : out_ref.shape[2]].reshape(out_ref.shape)


def on_device(sizes, hidden_state, filter_coefficients, meridian_offset_table, function_pick_table, observation, latitude_cosine_factor):
    nx, ny, nlat = sizes
    channels, band, columns = hidden_state.shape[1:]
    hbm = pl.BlockSpec(memory_space=pltpu.HBM)
    vmem = pl.BlockSpec(memory_space=pltpu.VMEM)
    row = pltpu.VMEM((8, LANES), F32)
    field = pltpu.VMEM((ROWS, LANES), HALO)
    edge = pltpu.VMEM((ROWS, TILE), HALO)
    raw = pltpu.VMEM((channels, band, columns), BF16)
    copies = 11 + 2 * (ny - 1) + 2 * ny * (nx - 1)
    gradient, weights = pl.pallas_call(
        functools.partial(kernel, nx, ny, nlat),
        out_shape=(
            jax.ShapeDtypeStruct((BASES * ROWS, LANES), BF16),
            jax.ShapeDtypeStruct((2 * channels, BASES * ROWS), BF16),
        ),
        in_specs=[hbm] * 7,
        out_specs=(vmem, vmem),
        scratch_shapes=[
            pltpu.SMEM((band, 3), jnp.int32),
            pltpu.SMEM((band,), F32),
            raw,
            pltpu.VMEM(filter_coefficients.shape, BF16),
            pltpu.VMEM(function_pick_table.shape, jnp.int32),
            pltpu.VMEM(observation.shape, F32),
            pltpu.VMEM((104, 18), BF16),
            pltpu.SemaphoreType.DMA((7,)),
            raw,
            pltpu.VMEM((2, 2 * channels, LANES), BF16),
            pltpu.VMEM((2, DEEP, LANES), BF16),
            pltpu.VMEM((2, DEEP, TILE), BF16),
            pltpu.VMEM((2, DEEP, LANES), BF16),
            pltpu.VMEM((2, DEEP, TILE), BF16),
            pltpu.VMEM((2 * ROWS, LANES), F32),
            pltpu.VMEM((2, 9, 3, 8, LANES), F32),
            pltpu.VMEM((2, 9, 3, 8, LANES), F32),
            pltpu.VMEM((2, 3, 8, LANES), F32),
            pltpu.VMEM((2, 9, 8, LANES), F32),
            pltpu.VMEM((2, 9, 8, LANES), F32),
            pltpu.VMEM((2, 9, 3, 8, LANES), F32),
            pltpu.VMEM((2, 9, 3, 8, LANES), F32),
            pltpu.VMEM((2, 9, 3, 8, LANES), F32),
            row, row, pltpu.VMEM((2, 8, LANES), F32),
            pltpu.VMEM((2, 9, 8, TILE), F32),
            pltpu.VMEM((2, 9, 8, TILE), F32),
            pltpu.VMEM((40, LANES), BF16),
            pltpu.VMEM((ny - 1, 40, LANES), BF16),
            pltpu.VMEM((ny, nx - 1, 40, LANES), BF16),
            pltpu.VMEM((2, 3, 8, TILE), F32),
            pltpu.VMEM((2, 3, 8, TILE), F32),
            field, field, pltpu.VMEM((2, ROWS, LANES), HALO),
            edge, edge, pltpu.VMEM((2, ROWS, TILE), HALO),
            pltpu.SemaphoreType.REGULAR,
            pltpu.SemaphoreType.DMA((copies,)),
            pltpu.SemaphoreType.DMA((copies,)),
        ],
        compiler_params=pltpu.CompilerParams(collective_id=0, has_side_effects=True, vmem_limit_bytes=16 << 20),
    )(
        *[
            pltpu.with_memory_space_constraint(array, pltpu.HBM)
            for array in (
                meridian_offset_table.T,
                latitude_cosine_factor,
                hidden_state.reshape(channels, band, columns),
                filter_coefficients,
                function_pick_table,
                observation,
                jnp.asarray(expand_picks(), BF16),
            )
        ]
    )
    out = pl.pallas_call(
        last_product,
        out_shape=jax.ShapeDtypeStruct((channels, band, columns), F32),
        in_specs=[vmem, vmem],
        out_specs=vmem,
        compiler_params=pltpu.CompilerParams(vmem_limit_bytes=16 << 20),
    )(weights, gradient)
    return out[None]


def solution(mesh):
    members = mesh.shape["ens"]
    nx = 4 if members % 4 == 0 and members > 4 else 2
    return jax.shard_map(
        functools.partial(on_device, (nx, members // nx, mesh.shape["lat"])),
        mesh=mesh,
        in_specs=(
            P("ens", None, "lat", "lon"),
            P(),
            P(None, "lat"),
            P(None, "lat", "lon"),
            P(None, "lat", "lon"),
            P("lat"),
        ),
        out_specs=P("ens", None, "lat", "lon"),
        check_vma=False,
    )
```

```python
import functools

import jax
import jax.numpy as jnp
import numpy as np
from jax import lax
from jax.experimental import pallas as pl
from jax.experimental.pallas import tpu as pltpu
from jax.sharding import PartitionSpec as P

SPAN = 4
BASES = 9
LANES = 384
TILE = 128
ROWS = 24
SMOOTH = 0.01
F32 = jnp.float32
BF16 = jnp.bfloat16
MESH = pl.DeviceIdType.MESH
HALO = BF16
DEEP = 96
PIECES = ((0, 40),)
ALONG_Y = (1, -1, 2)


def expand_picks():
    rows = np.zeros((104, 18), np.float32)
    for i in range(3):
        for sub in range(8):
            rows[8 * i + sub, 2 * (3 + i) + (sub & 1)] = 1
            rows[24 + 8 * i + sub, 2 * (6 + i) if sub & 1 else 2 * i + 1] = 1
            rows[48 + 8 * i + sub, 2 * (6 + i) + 1 if sub & 1 else 2 * i] = 1
        rows[72 + i, 2 * i] = 1
        rows[80 + i, 2 * (6 + i) + 1] = 1
        rows[88 + 3 + i, 2 * i] = 1
        rows[96 + 3 + i, 2 * (6 + i) + 1] = 1
    return rows


def iota(shape, dim):
    return lax.broadcasted_iota(jnp.int32, shape, dim)


def swapped(x):
    return jnp.where(iota(x.shape, x.ndim - 2) % 2 == 0, row_up(x), row_down(x))


def packed(pair):
    middle = jnp.where(iota((8, LANES), 0) < 4, pair[0][2], pltpu.roll(pair[1][2], 4, axis=0))
    return jnp.concatenate([pair[0][:2], middle[None], pair[1][:2]], axis=0)


def unpacked(x):
    return [x[:3], jnp.concatenate([x[3:], pltpu.roll(x[2], 4, axis=0)[None]], axis=0)]


def lane_roll(x, by):
    by %= x.shape[-1]
    return x if by == 0 else pltpu.roll(x, by, axis=x.ndim - 1)


def row_down(x):
    return pltpu.roll(x, 1, axis=x.ndim - 2)


def row_up(x):
    return pltpu.roll(x, x.shape[-2] - 1, axis=x.ndim - 2)


def smoothed_derivative(d):
    return d * lax.rsqrt(d * d + SMOOTH)


def shifted(pair, sign, steps):
    rolled = {}

    def at(parity, by):
        if (parity, by) not in rolled:
            rolled[parity, by] = lane_roll(pair[parity], -by)
        return rolled[parity, by]

    steps = jnp.broadcast_to(steps, pair[0].shape)
    out = []
    for parity in (0, 1):
        result = None
        for n in range(1, SPAN + 1):
            column = parity + sign * n
            value = at(column % 2, column // 2)
            result = value if result is None else jnp.where(steps == float(n), value, result)
        out.append(result)
    return out


def edge_of(x):
    lane = iota((*x.shape[:-1], TILE), x.ndim - 1)
    return jnp.where(lane < 64, x[..., :TILE], x[..., 2 * TILE :])


def extended(x, edge):
    lane = iota(edge.shape, edge.ndim - 1)
    last = jnp.where(
        lane < 104, x[..., 2 * TILE :], jnp.where(lane < 112, lane_roll(edge, 104), lane_roll(edge, 24))
    )
    return jnp.concatenate([x[..., : 2 * TILE], last], axis=-1)


def kernel(
    nx, ny, nlat, off_hbm, cos_hbm, x_hbm, w_hbm, pk_hbm, obs_hbm, ex_hbm, pg_ref, wb_ref,
    off_ref, cos_ref, x_raw, w_ref, pk_ref, obs_ref, ex_ref, in_sem, x_par, x_pad, x_row, x_rim, r_row, r_edge, obs_tmp,
    prod, far, qpf, qp, mask, csum, fsel, pgrad, su, sd, r_picks,
    qpe, rqpe, own, yblk, xblk, fe, rfe, f0, f1, r_grad, f0e, f1e, r_rim, ring_sem, send_sem, recv_sem,
):
    ens = lax.axis_index("ens")
    lat = lax.axis_index("lat")
    lon = lax.axis_index("lon")
    ex, ey = ens // ny, ens % ny
    has_up = (lat + nlat - 1) // nlat
    has_down = (2 * nlat - 2 - lat) // nlat
    partner = 1 - lon
    have_up = has_up.astype(F32)
    have_down = has_down.astype(F32)
    up = {"t": lat - has_up, "n": has_up * lon + (1 - has_up) * partner}
    down = {"t": lat + has_down, "n": has_down * lon + (1 - has_down) * partner}
    up_partner = {"t": lat - has_up, "n": partner}
    down_partner = {"t": lat + has_down, "n": partner}

    def x_peer(d):
        return ((ex + d) % nx) * ny + ey

    def y_peer(d):
        return ex * ny + (ey + d) % ny

    def target(e=None, t=None, n=None):
        return (ens if e is None else e, lat if t is None else t, lon if n is None else n)

    def step_of(a, q):
        return off_ref[q, a].astype(F32)

    sems = [0]

    def remote(src, dst, device):
        i = sems[0]
        sems[0] += 1
        return pltpu.make_async_remote_copy(
            src_ref=src, dst_ref=dst, send_sem=send_sem.at[i], recv_sem=recv_sem.at[i],
            device_id=device, device_id_type=MESH,
        )

    inputs = {}
    pairs = [
        ("x", x_hbm, x_raw), ("ex", ex_hbm, ex_ref), ("pk", pk_hbm, pk_ref), ("off", off_hbm, off_ref),
        ("w", w_hbm, w_ref), ("obs", obs_hbm, obs_ref), ("cos", cos_hbm, cos_ref),
    ]
    for i, (name, src, dst) in enumerate(pairs):
        inputs[name] = pltpu.make_async_copy(src, dst, in_sem.at[i])
        inputs[name].start()

    barrier = pltpu.get_barrier_semaphore()
    peers = [target(n=partner)]
    peers += [target(**where) for where in (up, down, up_partner, down_partner)]
    peers += [target(e=x_peer(d)) for d in (1, nx - 1)[: nx - 1]] + [target(e=y_peer(d)) for d in (1, ny - 1)[: ny - 1]]
    for device in peers:
        pl.semaphore_signal(barrier, inc=1, device_id=device, device_id_type=MESH)

    channels, latent_columns = x_raw.shape[0], x_raw.shape[2]
    latents = 2 * channels
    shape = (2 * DEEP, latents)
    wanted = jnp.where(iota(shape, 0) < DEEP, 2 * iota(shape, 0), 2 * (iota(shape, 0) - DEEP) + 1)
    wanted = jnp.where(wanted == iota(shape, 1), 1.0, 0.0).astype(BF16)
    for i in (0, 1):
        x_pad[i, :, 2 * TILE :] = jnp.zeros((latents, TILE), BF16)
    inputs["x"].wait()
    x_pad[0, :, :latent_columns] = x_raw[...].reshape(latents, latent_columns)
    split = jnp.dot(wanted, x_pad[0], preferred_element_type=F32)
    for r in (0, 1):
        row = split[DEEP * r : DEEP * (r + 1)]
        x_row[r] = row.astype(BF16)
        x_rim[r] = edge_of(row).astype(BF16)
    pl.semaphore_wait(barrier, len(peers))
    started = []

    def go(src, dst, device):
        copy = remote(src, dst, device)
        copy.start()
        started.append(copy)
        return copy

    def halo(to_up, to_down, into, where_up, where_down):
        base = sems[0]
        sems[0] += 2
        slots = [(to_up, where_up, has_up), (to_down, where_down, 1 - has_down)]
        arrivals = []
        for i, (src, where, slot) in enumerate(slots):
            def copy(index, src=src, where=where, i=i):
                return pltpu.make_async_remote_copy(
                    src_ref=src, dst_ref=into.at[index], send_sem=send_sem.at[base + i],
                    recv_sem=recv_sem.at[base + index], device_id=target(**where), device_id_type=MESH,
                )

            out = copy(slot)
            out.start()
            started.append(out)
            arrivals.append(copy(i))
        return arrivals

    if nx == 4:
        for device in (target(e=x_peer(1)), target(e=y_peer(1))):
            pl.semaphore_signal(ring_sem, inc=1, device_id=device, device_id_type=MESH)
    c_rims = halo(x_rim.at[0], x_rim.at[1], r_edge, up_partner, down_partner)
    c_rows = halo(x_row.at[0], x_row.at[1], r_row, up, down)
    c_x = go(x_raw, x_par, target(n=partner))

    pick = iota((256, 256), 0) - 2 * iota((256, 256), 1)
    half = iota((256, 256), 1)
    select = jnp.where((pick == jnp.where(half < TILE, 0, -255)), 1.0, 0.0).astype(BF16)
    columns = pk_ref.shape[2]
    widths = [slice(256 * block, min(256 * block + 256, columns)) for block in range(3)]
    inputs["ex"].wait()
    inputs["pk"].wait()
    picks = pk_ref[...].astype(F32).reshape(18, columns).astype(BF16)
    rows = jnp.dot(ex_ref[...], picks, preferred_element_type=F32).astype(BF16)
    inputs["off"].wait()
    row8 = iota((8, TILE), 0)
    for block in range(3):
        wide = widths[block]
        part = select[: wide.stop - wide.start]
        tile = slice(TILE * block, TILE * block + TILE)
        got = jnp.dot(rows[:, wide], part, preferred_element_type=F32)
        for slot in range(6):
            qp[0, slot, :, tile] = got[8 * slot : 8 * slot + 8, :TILE]
            qp[1, slot, :, tile] = got[8 * slot : 8 * slot + 8, TILE:]
        for slot in range(3):
            qpf[0, slot, :, tile] = got[48 + 8 * slot : 56 + 8 * slot, :TILE]
            qpf[1, slot, :, tile] = got[48 + 8 * slot : 56 + 8 * slot, TILE:]
        su[:, tile] = jnp.where(row8 == 6, step_of(0, 0), got[72:80, :TILE] + got[88:96, TILE:])
        sd[:, tile] = jnp.where(row8 == 6, step_of(2, 1), got[80:88, :TILE] + got[96:104, TILE:])
    c_picks = halo(su, sd, r_picks, up, down)

    inputs["w"].wait()
    one = jnp.where(iota((ROWS, 10), 0) // 2 == iota((ROWS, 10), 1), 1.0, 0.0).astype(BF16)
    spread = [jnp.dot(one, w_ref[k], preferred_element_type=F32) for k in range(BASES)]
    spread = jnp.concatenate(spread, axis=0).astype(BF16)
    shape = (w_ref.shape[2], latents)
    s2 = jnp.where(iota(shape, 1) // 2 == iota(shape, 0), 1.0, 0.0).astype(BF16)
    wf = jnp.dot(spread, s2, preferred_element_type=F32)
    wf = jnp.where(iota(wf.shape, 0) % 2 == iota(wf.shape, 1) % 2, wf, 0.0).astype(BF16)
    s2t = jnp.where(iota(shape[::-1], 0) // 2 == iota(shape[::-1], 1), 1.0, 0.0).astype(BF16)
    wb = lax.dot_general(s2t, spread, (((1,), (1,)), ((), ())), preferred_element_type=F32)
    wb_ref[...] = jnp.where(iota(wb.shape, 0) % 2 == iota(wb.shape, 1) % 2, wb, 0.0).astype(BF16)
    shape = (w_ref.shape[2], 2 * DEEP)
    s3 = jnp.where(iota(shape, 1) % DEEP == iota(shape, 0), 1.0, 0.0).astype(BF16)
    wn = jnp.dot(spread, s3, preferred_element_type=F32)
    wn = jnp.where((iota(wn.shape, 0) % 2 == 0) == (iota(wn.shape, 1) < DEEP), wn, 0.0).astype(BF16)

    inputs["obs"].wait()
    obs = obs_ref[...].reshape(20, columns)
    obs_hi = obs.astype(BF16)
    obs_lo = (obs - obs_hi.astype(F32)).astype(BF16)
    obs_tmp[...] = jnp.zeros_like(obs_tmp)
    for block in range(3):
        wide = widths[block]
        part = select[: wide.stop - wide.start]
        tile = slice(TILE * block, TILE * block + TILE)
        both = jnp.dot(obs_hi[:, wide], part, preferred_element_type=F32) + jnp.dot(
            obs_lo[:, wide], part, preferred_element_type=F32
        )
        obs_tmp[: obs.shape[0], tile] = both[:, :TILE]
        obs_tmp[ROWS : ROWS + obs.shape[0], tile] = both[:, TILE:]
    inputs["cos"].wait()

    c_x.wait_recv()
    x_pad[1, :, :latent_columns] = x_par[...].reshape(latents, latent_columns)
    sector = [x_pad[i].astype(F32) for i in (0, 1)]
    latent = extended(sector[0], edge_of(sector[1]))
    halfway = 0.5 * (latent + lane_roll(latent, -1))
    for parity, x in enumerate((latent, halfway)):
        got = jnp.dot(wf, x.astype(BF16), preferred_element_type=F32)
        prod[parity] = got.reshape(BASES, 3, 8, LANES)

    even = iota((8, LANES), 0) % 2 == 0
    even3 = iota((3, 8, LANES), 1) % 2 == 0
    steps = [
        jnp.where(even, step_of(1, 0), step_of(1, 1)),
        jnp.where(even, step_of(0, 1), step_of(2, 0)),
        jnp.where(even, step_of(0, 0), step_of(2, 1)),
    ]

    def build_masks(kind, source):
        for b in (-1, 0, 1):
            slot = 3 * kind + b + 1
            pair = source(slot)
            if b:
                pair = shifted(pair, -b, steps[kind])
            for parity in (0, 1):
                mask[parity, slot] = pair[parity]

    def own_columns(slot):
        return [qp[0, slot], qp[1, slot]]

    def all_columns(slot):
        return [extended(qp[parity, slot], rqpe[parity, slot]) for parity in (0, 1)]

    def pick_products(product, slots):
        for parity in (0, 1):
            for t in range(3):
                tile = slice(TILE * t, TILE * t + TILE)
                values = [product[parity, k, :, :, tile] for k in range(BASES)]
                for slot in slots:
                    want = jnp.broadcast_to(mask[parity, slot, :, tile][None], (3, 8, TILE))
                    total = jnp.where(want == 0.0, values[0], 0.0)
                    for k in range(1, BASES):
                        total = jnp.where(want == float(k), values[k], total)
                    csum[parity, slot, :, :, tile] = total

    def target_sum(kind):
        total = [csum[0, 3 * kind + 1], csum[1, 3 * kind + 1]]
        for b in (-1, 1):
            slot = 3 * kind + b + 1
            moved = shifted([csum[0, slot], csum[1, slot]], b, steps[kind])
            total = [x + y for x, y in zip(total, moved)]
        return total

    for kind in (0, 1):
        build_masks(kind, own_columns)
    pick_products(prod, range(6))
    local = [x + swapped(y) for x, y in zip(target_sum(0), target_sum(1))]
    build_masks(2, lambda slot: [qpf[0, slot - 6], qpf[1, slot - 6]])

    for copy in c_rows + c_rims:
        copy.wait_recv()
    around_x = extended(
        r_row[...].reshape(2 * DEEP, LANES).astype(F32), r_edge[...].reshape(2 * DEEP, TILE).astype(F32)
    )
    for parity, x in enumerate((around_x, 0.5 * (around_x + lane_roll(around_x, -1)))):
        far[parity] = jnp.dot(wn, x.astype(BF16), preferred_element_type=F32).reshape(BASES, 3, 8, LANES)
    pick_products(far, range(6, 9))
    present = jnp.where(even3, have_up, have_down)
    pred = [x + present * y for x, y in zip(local, target_sum(2))]
    mine = packed(pred)
    own[...] = mine.reshape(40, LANES).astype(BF16)

    def spread_row(i):
        return jnp.where(
            even,
            jnp.broadcast_to(r_picks[0, i : i + 1, :], (8, LANES)),
            jnp.broadcast_to(r_picks[1, i : i + 1, :], (8, LANES)),
        )

    def backward_masks():
        for copy in c_picks:
            copy.wait_recv()
        steps[2] = spread_row(6)
        for parity in (0, 1):
            for i in range(3):
                qp[parity, 6 + i] = spread_row(3 * parity + i)
            qpe[parity] = edge_of(qp[parity])
        go(qpe, rqpe, target(n=partner)).wait_recv()
        for kind in range(3):
            build_masks(kind, all_columns)

    def terms(ref):
        return smoothed_derivative(mine - ref[...].astype(F32).reshape(5, 8, LANES))

    if nx == 4:
        ring = (1, -1, 2)

        def slot(dx, dy, rows):
            place = xblk.at[ring.index(dy) + 1 if dy else 0, ring.index(dx)] if dx else yblk.at[ring.index(dy)]
            return place.at[pl.ds(*rows)]

        pl.semaphore_wait(ring_sem, 2)
        arrivals = {}
        for rows in PIECES:
            for dy in ALONG_Y:
                arrivals[0, dy, rows] = go(own.at[pl.ds(*rows)], slot(0, dy, rows), target(e=y_peer(dy % ny)))
        for rows in PIECES:
            for dx in ring:
                arrivals[dx, 0, rows] = go(own.at[pl.ds(*rows)], slot(dx, 0, rows), target(e=x_peer(dx % nx)))
        backward_masks()
        for rows in PIECES:
            for dy in ring:
                arrivals[0, dy, rows].wait_recv()
                for dx in (2, 1, -1):
                    arrivals[dx, dy, rows] = go(slot(0, dy, rows), slot(dx, dy, rows), target(e=x_peer(dx % nx)))
        pair_total = jnp.zeros_like(mine)
        for dy in (0, *ring):
            if dy:
                pair_total += terms(yblk.at[ring.index(dy)])
            for dx in ring:
                for rows in PIECES:
                    arrivals[dx, dy, rows].wait_recv()
                pair_total += terms(xblk.at[ring.index(dy) + 1 if dy else 0, ring.index(dx)])
    else:
        c_y = [go(own, yblk.at[d - 1], target(e=y_peer(d))) for d in range(1, ny)]
        relayed = [[go(own, xblk.at[0, d - 1], target(e=x_peer(d))) for d in range(1, nx)]]
        pair_total = jnp.zeros_like(mine)
        for d in range(1, ny):
            c_y[d - 1].wait_recv()
            relayed.append([go(yblk.at[d - 1], xblk.at[d, e - 1], target(e=x_peer(e))) for e in range(1, nx)])
            pair_total += terms(yblk.at[d - 1])
        backward_masks()
        for d in range(ny):
            for e in range(1, nx):
                relayed[d][e - 1].wait_recv()
                pair_total += terms(xblk.at[d, e - 1])
    pair_total = unpacked(pair_total)

    factor = jnp.where(even3, cos_ref[0], cos_ref[1])
    grad = []
    for parity in (0, 1):
        miss = pred[parity] - obs_tmp[ROWS * parity : ROWS * (parity + 1)].reshape(3, 8, LANES)
        grad.append(factor * (smoothed_derivative(miss) - pair_total[parity] * (1.0 / (nx * ny - 1))))
        fe[parity] = edge_of(grad[parity])
    lower = jnp.where(even3, grad[0], row_down(grad[1]))
    upper = jnp.where(even3, row_up(grad[0]), grad[1])
    f0[...] = lower.reshape(ROWS, LANES).astype(f0.dtype)
    f1[...] = upper.reshape(ROWS, LANES).astype(f1.dtype)
    f0e[...] = edge_of(lower).reshape(ROWS, TILE).astype(f0e.dtype)
    f1e[...] = edge_of(upper).reshape(ROWS, TILE).astype(f1e.dtype)
    c_fe = go(fe, rfe, target(n=partner))
    c_f = halo(f0, f1, r_grad, up, down) + halo(f0e, f1e, r_rim, up_partner, down_partner)

    def spread_gradient(kind, wide):
        for b in (-1, 0, 1):
            pair = shifted(wide, -b, steps[kind]) if b else wide
            for parity in (0, 1):
                fsel[parity, 3 * kind + b + 1] = pair[parity]

    def add_gradient(slots, first):
        for parity in (0, 1):
            for t in range(3):
                tile = slice(TILE * t, TILE * t + TILE)
                values = [fsel[parity, slot, :, :, tile] for slot in slots]
                wants = [jnp.broadcast_to(mask[parity, slot, :, tile][None], (3, 8, TILE)) for slot in slots]
                for k in range(BASES):
                    chosen = [jnp.where(want == float(k), value, 0.0) for want, value in zip(wants, values)]
                    if not first:
                        chosen.append(pgrad[parity, k, :, :, tile])
                    while len(chosen) > 1:
                        chosen = [x + y for x, y in zip(chosen[::2], chosen[1::2])] + chosen[len(chosen) & ~1 :]
                    pgrad[parity, k, :, :, tile] = chosen[0]

    c_fe.wait_recv()
    wide = [extended(grad[parity], rfe[parity]) for parity in (0, 1)]
    spread_gradient(0, wide)
    spread_gradient(1, [swapped(x) for x in wide])
    add_gradient(range(6), True)

    def neighbours(below, above):
        below = below.astype(F32).reshape(3, 8, -1) * have_down
        above = above.astype(F32).reshape(3, 8, -1) * have_up
        is_even = iota(below.shape, 1) % 2 == 0
        return [jnp.where(is_even, above, row_down(below)), jnp.where(is_even, row_up(above), below)]

    for copy in c_f:
        copy.wait_recv()
    inner, rim = neighbours(r_grad[1], r_grad[0]), neighbours(r_rim[1], r_rim[0])
    spread_gradient(2, [extended(x, edge) for x, edge in zip(inner, rim)])
    add_gradient(range(6, 9), False)

    odd = pgrad[1].reshape(BASES * ROWS, LANES)
    folded = pgrad[0].reshape(BASES * ROWS, LANES) + 0.5 * (odd + lane_roll(odd, 1))
    pg_ref[...] = folded.astype(BF16)

    for copy in started:
        copy.wait_send()


def last_product(wb_ref, pg_ref, out_ref):
    got = jnp.dot(wb_ref[...], pg_ref[...], preferred_element_type=F32)
    out_ref[...] = got[:, : out_ref.shape[2]].reshape(out_ref.shape)


def on_device(sizes, hidden_state, filter_coefficients, meridian_offset_table, function_pick_table, observation, latitude_cosine_factor):
    nx, ny, nlat = sizes
    channels, band, columns = hidden_state.shape[1:]
    hbm = pl.BlockSpec(memory_space=pltpu.HBM)
    vmem = pl.BlockSpec(memory_space=pltpu.VMEM)
    row = pltpu.VMEM((8, LANES), F32)
    field = pltpu.VMEM((ROWS, LANES), HALO)
    edge = pltpu.VMEM((ROWS, TILE), HALO)
    raw = pltpu.VMEM((channels, band, columns), BF16)
    copies = 11 + 2 * (ny - 1) + 2 * ny * (nx - 1)
    gradient, weights = pl.pallas_call(
        functools.partial(kernel, nx, ny, nlat),
        out_shape=(
            jax.ShapeDtypeStruct((BASES * ROWS, LANES), BF16),
            jax.ShapeDtypeStruct((2 * channels, BASES * ROWS), BF16),
        ),
        in_specs=[hbm] * 7,
        out_specs=(vmem, vmem),
        scratch_shapes=[
            pltpu.SMEM((band, 3), jnp.int32),
            pltpu.SMEM((band,), F32),
            raw,
            pltpu.VMEM(filter_coefficients.shape, BF16),
            pltpu.VMEM(function_pick_table.shape, jnp.int32),
            pltpu.VMEM(observation.shape, F32),
            pltpu.VMEM((104, 18), BF16),
            pltpu.SemaphoreType.DMA((7,)),
            raw,
            pltpu.VMEM((2, 2 * channels, LANES), BF16),
            pltpu.VMEM((2, DEEP, LANES), BF16),
            pltpu.VMEM((2, DEEP, TILE), BF16),
            pltpu.VMEM((2, DEEP, LANES), BF16),
            pltpu.VMEM((2, DEEP, TILE), BF16),
            pltpu.VMEM((2 * ROWS, LANES), F32),
            pltpu.VMEM((2, 9, 3, 8, LANES), F32),
            pltpu.VMEM((2, 9, 3, 8, LANES), F32),
            pltpu.VMEM((2, 3, 8, LANES), F32),
            pltpu.VMEM((2, 9, 8, LANES), F32),
            pltpu.VMEM((2, 9, 8, LANES), F32),
            pltpu.VMEM((2, 9, 3, 8, LANES), F32),
            pltpu.VMEM((2, 9, 3, 8, LANES), F32),
            pltpu.VMEM((2, 9, 3, 8, LANES), F32),
            row, row, pltpu.VMEM((2, 8, LANES), F32),
            pltpu.VMEM((2, 9, 8, TILE), F32),
            pltpu.VMEM((2, 9, 8, TILE), F32),
            pltpu.VMEM((40, LANES), BF16),
            pltpu.VMEM((ny - 1, 40, LANES), BF16),
            pltpu.VMEM((ny, nx - 1, 40, LANES), BF16),
            pltpu.VMEM((2, 3, 8, TILE), F32),
            pltpu.VMEM((2, 3, 8, TILE), F32),
            field, field, pltpu.VMEM((2, ROWS, LANES), HALO),
            edge, edge, pltpu.VMEM((2, ROWS, TILE), HALO),
            pltpu.SemaphoreType.REGULAR,
            pltpu.SemaphoreType.DMA((copies,)),
            pltpu.SemaphoreType.DMA((copies,)),
        ],
        compiler_params=pltpu.CompilerParams(collective_id=0, has_side_effects=True, vmem_limit_bytes=16 << 20),
    )(
        *[
            pltpu.with_memory_space_constraint(array, pltpu.HBM)
            for array in (
                meridian_offset_table.T,
                latitude_cosine_factor,
                hidden_state.reshape(channels, band, columns),
                filter_coefficients,
                function_pick_table,
                observation,
                jnp.asarray(expand_picks(), BF16),
            )
        ]
    )
    out = pl.pallas_call(
        last_product,
        out_shape=jax.ShapeDtypeStruct((channels, band, columns), F32),
        in_specs=[vmem, vmem],
        out_specs=vmem,
        compiler_params=pltpu.CompilerParams(vmem_limit_bytes=16 << 20),
    )(weights, gradient)
    return out[None]


def solution(mesh):
    members = mesh.shape["ens"]
    nx = 4 if members % 4 == 0 and members > 4 else 2
    return jax.shard_map(
        functools.partial(on_device, (nx, members // nx, mesh.shape["lat"])),
        mesh=mesh,
        in_specs=(
            P("ens", None, "lat", "lon"),
            P(),
            P(None, "lat"),
            P(None, "lat", "lon"),
            P(None, "lat", "lon"),
            P("lat"),
        ),
        out_specs=P("ens", None, "lat", "lon"),
        check_vma=False,
    )
```
